512 devices in a mesh: dp: 8 (over y), row: 4 (over x), col: 16 (over z, core).
Axes of the slice: x: 4, y: 8, z: 8, core: 2. Of those that a mesh axis runs over, the one named last changes fastest.
Arguments:
- tokens: bfloat16 [8192, 8192], P(('dp', 'col'), 'row'), may hold values from -6 to 6
- frozen_weight: bfloat16 [8192, 8192], P('row', 'col'), may hold values from -0.0625 to 0.0625
- input_adapter_factor: bfloat16 [16, 8192], P(None, 'row'), may hold values from -0.0625 to 0.0625
- output_adapter_factor: bfloat16 [16, 8192], P(None, 'col'), may hold values from -1.5 to 1.5
- magnitude: float32 [8192], P('col'), may hold values from 0.5 to 2
- cotangent: bfloat16 [8192, 8192], P(('dp', 'row'), 'col'), may hold values from -6 to 6
- sequence_lengths: int32 [8, 8], P('dp'), may hold values from 1 to 512, 1024 in all within a row
Outputs:
- projected: bfloat16 [8192, 8192], P(('dp', 'row'), 'col')
- grad_mag: float32 [8192], P('col')
- input_factor_gradient: float32 [16, 8192], P(None, 'row')
- grad_b: float32 [16, 8192], P(None, 'col')
The draws below stay inside these ranges and needn't reach their ends.
Inputs may be any that keep to these rules, and one draw needn't show every extreme that they name: `sequence_lengths`: each group's 8 lengths sum to 1024, and one of them is exactly 512.
All inputs are finite; a program needn't handle non-finite values.
Results may differ from the reference program's by a relative error of at most 0.0052.
Values may be sent and summed in bfloat16 or wider, within the bound.
A program may use at most 64 MiB of HBM per device.

```python
import math
import jax
import jax.numpy as jnp
import numpy as np
from jax import lax

MODEL_WIDTH = 8192
ADAPTER_RANK = 16
TOK = 1024
SEQS = 8
LONGEST = 512
GROUPS = 8
TOKENS = 8192


def levels(stream_key, dims, cuts, least, largest):
    gain = 1.0
    for position, parts in cuts:
        heights = jax.random.uniform(jax.random.fold_in(jax.random.fold_in(stream_key, 6), position), (parts,), jnp.float32, least / len(cuts), largest / len(cuts))
        gain = gain * jnp.repeat(jnp.exp(heights), dims[position] // parts).reshape((-1,) + (1,) * (len(dims) - 1 - position))
    return gain


def length_profile(count, total, reach, lean):
    weights = [(1 << 20) // math.isqrt(rank ** lean) + 1 for rank in range(2, count + 1)]
    rest, holding = total - reach - (count - 1), [1] * (count - 1)
    while rest > 0:
        free = [i for i in range(count - 1) if holding[i] < reach]
        mass, left = sum([weights[i] for i in free]), rest
        for i in free:
            extra = min(reach - holding[i], max(1, left * weights[i] // mass), rest)
            holding[i] = holding[i] + extra
            rest = rest - extra
    return np.array([reach] + holding)


def uneven(rng, amount, total, limit, skew):
    if amount == 2:
        one = jax.random.randint(rng, (), max(1, total - limit), min(limit, total - 1) + 1)
        return jnp.stack([one, total - one])
    sizes = jnp.asarray(length_profile(amount, total, limit, skew), jnp.int32)
    couples = (amount - 1) // 2
    donor, sink = sizes[1:1 + 2 * couples:2], sizes[2:2 + 2 * couples:2]
    slack = jnp.minimum(donor - 1, limit - sink)
    shifted = jax.random.randint(jax.random.fold_in(rng, 1), (couples,), 0, 1 << 20) % (slack + 1)
    sizes = sizes.at[1:1 + 2 * couples:2].set(donor - shifted).at[2:2 + 2 * couples:2].set(sink + shifted)
    return sizes[jax.random.permutation(jax.random.fold_in(rng, 2), amount)]


def centred(own_key, shape, deviation, bound, pieces=(), held_as=jnp.bfloat16):
    gain = levels(own_key, shape, pieces, -0.22, 0.18) if pieces else 1.0
    result = jax.random.normal(own_key, shape, jnp.float32) * deviation * gain
    return jnp.minimum(jnp.maximum(result, -bound), bound).astype(held_as)


def setup_inputs(seed: int = 0) -> dict:
    keys = jax.random.split(jax.random.key(seed), 8)
    tokens = centred(keys[0], (TOKENS, MODEL_WIDTH), 1.0, 6.0, ((0, 128), (1, 4)))
    frozen_weight = centred(keys[1], (MODEL_WIDTH, MODEL_WIDTH), MODEL_WIDTH ** -0.5, 0.0625, ((0, 4), (1, 16)))
    input_adapter_factor = centred(keys[2], (ADAPTER_RANK, MODEL_WIDTH), MODEL_WIDTH ** -0.5, 0.0625, ((1, 4),))
    output_adapter_factor = centred(keys[3], (ADAPTER_RANK, MODEL_WIDTH), ADAPTER_RANK ** -0.5, 1.5, ((1, 16),))
    magnitude = jnp.clip(jnp.exp(math.log(2.0) - 1.3862944 * jax.random.uniform(keys[4], (MODEL_WIDTH,), jnp.float32) ** levels(keys[4], (MODEL_WIDTH,), ((0, 16),), -0.2, 0.2)), 0.5, 2.0)
    cotangent = centred(keys[5], (TOKENS, MODEL_WIDTH), 1.0, 6.0, ((0, 32), (1, 16)))
    sequence_lengths = jax.vmap(lambda own: uneven(own, SEQS, TOK, LONGEST, 2))(jax.random.split(keys[6], GROUPS)).reshape((GROUPS, SEQS)).astype(jnp.int32)
    return dict(tokens=tokens, frozen_weight=frozen_weight, input_adapter_factor=input_adapter_factor, output_adapter_factor=output_adapter_factor, magnitude=magnitude, cotangent=cotangent, sequence_lengths=sequence_lengths)


norm_eps = 1e-06
highest_precision = lax.Precision.HIGHEST

def contract_product(left, right, left_dim, right_dim):
    return lax.dot_general(left, right, (((left_dim,), (right_dim,)), ((), ())), preferred_element_type=jnp.float32)

def token_weights(lengths, positions):
    ends = jnp.cumsum(lengths, dtype=jnp.int32)
    starts = ends - lengths
    inside = (positions[:, None] >= starts[None, :]) & (positions[:, None] < ends[None, :])
    inverse = 1.0 / lengths.astype(jnp.float32)
    return lax.optimization_barrier(jnp.sum(jnp.where(inside, inverse[None, :], jnp.float32(0.0)), axis=1))

def reference(tokens, frozen_weight, input_adapter_factor, output_adapter_factor, magnitude, cotangent, sequence_lengths):
    low_rank_update = contract_product(input_adapter_factor, output_adapter_factor, 0, 0)
    merged = frozen_weight.astype(jnp.float32) + low_rank_update
    col_norm = jnp.sqrt(lax.optimization_barrier(jnp.sum(merged * merged, axis=0)) + norm_eps)
    col_scale = magnitude / col_norm
    down_activations = contract_product(tokens, input_adapter_factor, 1, 1).astype(jnp.bfloat16)
    query_projection = jnp.dot(tokens, frozen_weight, preferred_element_type=jnp.float32) + jnp.dot(down_activations, output_adapter_factor, preferred_element_type=jnp.float32)
    projected = (query_projection * col_scale[None, :]).astype(jnp.bfloat16)
    positions = jnp.arange(TOK, dtype=jnp.int32)
    weights = jax.vmap(lambda lengths: token_weights(lengths, positions))(sequence_lengths).reshape(-1)
    grad_out = cotangent.astype(jnp.float32) * weights[:, None]
    scale_grad = lax.optimization_barrier(jnp.sum(grad_out * query_projection, axis=0))
    grad_mag = scale_grad / col_norm
    norm_coefficient = -scale_grad * magnitude / (col_norm * col_norm * col_norm)
    projection_gradient = (grad_out * col_scale[None, :]).astype(jnp.bfloat16)
    gram_product_matrix = contract_product(input_adapter_factor, input_adapter_factor, 1, 1)
    merged_input_factor = jnp.dot(input_adapter_factor, frozen_weight, preferred_element_type=jnp.float32) + jnp.dot(gram_product_matrix, output_adapter_factor.astype(jnp.float32), precision=highest_precision)
    grad_b = contract_product(down_activations, projection_gradient, 0, 0) + merged_input_factor * norm_coefficient[None, :]
    backward_rows = contract_product(projection_gradient, output_adapter_factor, 1, 1).astype(jnp.bfloat16)
    scaled_output_factor = (output_adapter_factor.astype(jnp.float32) * norm_coefficient[None, :]).astype(jnp.bfloat16)
    input_factor_gradient = contract_product(backward_rows, tokens, 0, 0) + contract_product(scaled_output_factor, frozen_weight, 1, 1)
    input_factor_gradient = input_factor_gradient + jnp.dot(contract_product(scaled_output_factor, output_adapter_factor, 1, 1), input_adapter_factor.astype(jnp.float32), precision=highest_precision)
    return (projected, grad_mag, input_factor_gradient, grad_b)
```

```python
import functools

import jax
import jax.numpy as jnp
from jax import lax
from jax.experimental import pallas as pl
from jax.experimental.pallas import tpu as pltpu
from jax.sharding import Mesh
from jax.sharding import PartitionSpec as P

AXES = ("dp", "row", "z", "core")
COL = ("z", "core")
EPS = 1e-06
F32 = jnp.float32
BF16 = jnp.bfloat16
HIGHEST = lax.Precision.HIGHEST


def nn(a, b):
    return lax.dot_general(a, b, (((1,), (0,)), ((), ())), preferred_element_type=F32)


def nt(a, b):
    return lax.dot_general(a, b, (((1,), (1,)), ((), ())), preferred_element_type=F32)


def tn(a, b):
    return lax.dot_general(a, b, (((0,), (0,)), ((), ())), preferred_element_type=F32)


def exact(a, b):
    return lax.dot_general(
        a, b, (((1,), (0,)), ((), ())), preferred_element_type=F32, precision=HIGHEST
    )


def fold(a):
    return jnp.sum(a.reshape(a.shape[0] // 8, 8, a.shape[1]), axis=0)


def kernel(
    sizes,
    tok_hbm, w_hbm, a_hbm, b_hbm, mag_ref, ct_hbm, lens_ref,
    proj_ref, gmag_ref, ifg_ref, gb_ref,
    T, W, A, B, CT, WT, PF, PS, PR, DB,
    NX, AX, SACC, SX, SY, SCALE, NORM, BG, BGS, BX, BY, R, RY, H, CX, ZX, AM,
    load_sem, zr_s, zr_r, zl_s, zl_r, dr_s, dr_r, dl_s, dl_r, do_s, do_r,
    ct_s, ct_r, p_s, p_r, nx_s, nx_r, ax_s, ax_r, sx_s, sx_r, sy_s, sy_r,
    bx_s, bx_r, by_s, by_r, bo_s, bo_r, ry_s, ry_r, cx_s, cx_r, zx_s, zx_r,
    yo_s, yo_r, co_s, co_r,
):
    ny, nx, nz = sizes
    y, x, z, k = (lax.axis_index(a) for a in AXES)
    rows = tok_hbm.shape[0]
    half = rows // 2
    unit = 2 * rows
    own = nz // nx * unit
    per = nz // nx
    slab = T.shape[1] // ny
    lane = slab // 2
    part = W.shape[1] // nx

    def at(axis, index):
        return tuple(index if i == axis else v for i, v in enumerate((y, x, z, k)))

    def step(axis, by, n):
        return at(axis, lax.rem((y, x, z)[axis] + by + n, n))

    partner = (y, x, z, 1 - k)
    right = step(2, 1, nz)
    left = step(2, -1, nz)

    def copy(src, dst, ssem, rsem, dev):
        return pltpu.make_async_remote_copy(
            src_ref=src, dst_ref=dst, send_sem=ssem, recv_sem=rsem,
            device_id=dev, device_id_type=pl.DeviceIdType.MESH,
        )

    barrier = pltpu.get_barrier_semaphore()
    greeted = 0
    for axis, n in ((0, ny), (1, nx), (2, nz)):
        for d in range(1, n):
            pl.semaphore_signal(
                barrier, inc=1, device_id=step(axis, d, n), device_id_type=pl.DeviceIdType.MESH
            )
            greeted += 1
    pl.semaphore_signal(barrier, inc=1, device_id=partner, device_id_type=pl.DeviceIdType.MESH)
    greeted += 1

    def token_rows(chip, core, h, n):
        return pl.ds(pl.multiple_of(chip * unit + core * rows + h * half, half), n)

    mine = token_rows(z, k, 0, rows)
    owned = pl.ds(pl.multiple_of(x * own, own), own)
    loads = [
        pltpu.make_async_copy(tok_hbm, T.at[mine], load_sem.at[0]),
        pltpu.make_async_copy(ct_hbm, CT.at[owned], load_sem.at[1]),
        pltpu.make_async_copy(a_hbm, A, load_sem.at[2]),
        pltpu.make_async_copy(b_hbm, B, load_sem.at[3]),
        pltpu.make_async_copy(w_hbm, W, load_sem.at[4]),
    ]
    for c in loads:
        c.start()

    seqs = lens_ref.shape[1]

    def weigh(i, _):
        pos = lax.broadcasted_iota(jnp.int32, (unit, 128), 0) + i * unit
        total = jnp.zeros((unit, 128), F32)
        start = jnp.int32(0)
        for s in range(seqs):
            length = lens_ref[0, s]
            end = start + length
            inverse = 1.0 / jnp.full((1, 128), length, jnp.int32).astype(F32)
            total += jnp.where((pos >= start) & (pos < end), inverse, 0.0)
            start = end
        WT[pl.ds(pl.multiple_of(i * unit, unit), unit), :] = total
        return 0

    lax.fori_loop(0, nz, weigh, 0)

    loads[0].wait()
    loads[1].wait()
    pl.semaphore_wait(barrier, greeted)

    def ring(right_way, src_chip, h, idx):
        r = token_rows(src_chip, k, h, half)
        if right_way:
            return copy(T.at[r], T.at[r], zr_s.at[idx], zr_r.at[idx], right)
        return copy(T.at[r], T.at[r], zl_s.at[idx], zl_r.at[idx], left)

    def across(right_way, src_chip, core, h, idx):
        r = token_rows(src_chip, core, h, half)
        if right_way:
            return copy(T.at[r], T.at[r], dr_s.at[idx], dr_r.at[idx], partner)
        return copy(T.at[r], T.at[r], dl_s.at[idx], dl_r.at[idx], partner)

    def across_own(core):
        r = token_rows(z, core, 0, rows)
        return copy(T.at[r], T.at[r], do_s.at[0], do_r.at[0], partner)

    steps = nz // 2
    last = 2 * steps - 2
    ring(True, z, 0, 0).start()
    ring(False, z, 0, 0).start()
    ring(True, z, 1, 1).start()
    ring(False, z, 1, 1).start()
    across_own(k).start()

    def chip_of(j):
        s = (j + 1) // 2
        return lax.rem(z + nz + jnp.where(lax.rem(j, 2) == 1, -s, s), nz)

    def unit_rows(chip):
        return pl.ds(pl.multiple_of(chip * unit, unit), unit)

    def ct_copy(chip, d):
        r = unit_rows(chip)
        return copy(
            CT.at[r], CT.at[r], ct_s.at[(d - 1) * per + lax.rem(chip, per)], ct_r.at[chip],
            step(1, d, nx),
        )

    def send_ct(j, _):
        chip = chip_of(j)

        @pl.when(chip // per == x)
        def _():
            for d in range(1, nx):
                ct_copy(chip, d).start()

        return 0

    for c in loads[2:]:
        c.wait()
    chunk = slab

    def norm_part(i, acc):
        c = pl.ds(pl.multiple_of(i * chunk, chunk), chunk)
        m = W[c, :].astype(F32) + tn(A[:, c], B[...])
        return acc + fold(m * m)

    acc = lax.fori_loop(0, ny, norm_part, jnp.zeros((8, W.shape[1]), F32))
    NX[x] = jnp.sum(acc, axis=0, keepdims=True)

    def to_x(src, slot, ssem, rsem, d):
        return copy(src, slot, ssem.at[d - 1], rsem.at[x], step(1, d, nx))

    def from_x(slots, rsem, ssem, d):
        src = lax.rem(x + d, nx)
        return copy(slots.at[src], slots.at[src], ssem.at[d - 1], rsem.at[src], step(1, d, nx))

    for d in range(1, nx):
        to_x(NX.at[x], NX.at[x], nx_s, nx_r, d).start()
    lax.fori_loop(0, nz, send_ct, 0)

    am = nn(A[...], W[...]) + exact(nt(A[...], A[...]), B[...].astype(F32))
    for i in range(nx):
        AM[i] = am[:, i * part : (i + 1) * part]

    SACC[...] = jnp.zeros_like(SACC)
    BG[...] = jnp.zeros_like(BG)
    R[...] = jnp.zeros_like(R)

    for d in range(1, nx):
        dst = lax.rem(x + d, nx)
        copy(AM.at[dst], AX.at[x], ax_s.at[d - 1], ax_r.at[x], step(1, d, nx)).start()
    AX[x] = AM[x]

    def project(chip):
        r = unit_rows(chip)
        t = T[r, :]
        down = nt(t, A[...]).astype(BF16)
        p = nn(t, W[...]) + nn(down, B[...])
        DB[r, :] = down
        PF[r, :] = p
        PS[r, :] = p.astype(BF16)

    def need_ct(chip):
        @pl.when(chip // per != x)
        def _():
            ct_copy(chip, 1).wait_recv()

    def weighted(chip):
        r = unit_rows(chip)
        w = WT[r, :]
        return CT[r, :].astype(F32) * jnp.concatenate([w] * (W.shape[1] // 128), axis=1)

    def scale_sum(chip):
        SACC[...] += fold(weighted(chip) * PF[unit_rows(chip), :])

    def backward(chip):
        r = unit_rows(chip)
        gp = (weighted(chip) * SCALE[...]).astype(BF16)
        BG[...] += tn(DB[r, :], gp)
        back = nt(B[...], gp)
        high = back.astype(BF16)
        low = (back - high.astype(F32)).astype(BF16)
        both = nn(jnp.concatenate([high, low], axis=0), T[r, :])
        R[...] += both[: back.shape[0]] + both[back.shape[0] :]

    def p_copy(chip, src, dst):
        loc = lax.rem(chip, per)
        r = pl.ds(pl.multiple_of(loc * unit, unit), unit)
        return copy(
            PS.at[unit_rows(chip)], PR.at[src, r], p_s.at[chip], p_r.at[src * per + loc], at(1, dst)
        )

    def send_p(chip):
        @pl.when(chip // per != x)
        def _():
            p_copy(chip, x, chip // per).start()

    def handle(i):
        s = i // 2 + 1
        h = lax.rem(i, 2)
        hr = h
        hl = jnp.where(i == last, 1, h)
        fr = lax.rem(z - s + nz, nz)
        fl = lax.rem(z + s, nz)
        ring(True, fr, hr, i).wait_recv()

        @pl.when(i < last - 1)
        def _():
            ring(True, fr, hr, i + 2).start()

        across(True, fr, k, hr, i).start()
        ring(False, fl, hl, i).wait_recv()

        @pl.when((i < last - 2) | (i == last - 1))
        def _():
            ring(False, fl, hl, jnp.where(i == last - 1, last, i + 2)).start()

        across(False, fl, k, hl, i).start()

    def need_tokens(j):
        @pl.when(j == 0)
        def _():
            across_own(1 - k).wait_recv()

        s = (j + 1) // 2

        @pl.when((lax.rem(j, 2) == 1) & (j < nz - 1))
        def _():
            for h in range(2):
                across(True, chip_of(j), 1 - k, h, j - 1 + h).wait_recv()

        @pl.when((lax.rem(j, 2) == 0) & (j > 0))
        def _():
            for h in range(2):
                across(False, chip_of(j), 1 - k, h, j - 2 + h).wait_recv()

        @pl.when(j == nz - 1)
        def _():
            across(True, chip_of(j), 1 - k, 0, last).wait_recv()
            across(False, chip_of(j), 1 - k, 1, last).wait_recv()

    lag = 2
    held = nz - 3

    def turn(j, _):
        chip = chip_of(j)
        need_tokens(j)
        project(chip)

        @pl.when(j == 1)
        def _():
            for d in range(1, nx):
                from_x(NX, nx_r, nx_s, d).wait_recv()
            sq = NX[0]
            for i in range(1, nx):
                sq = sq + NX[i]
            norm = jnp.sqrt(sq + EPS)
            NORM[...] = norm
            SCALE[...] = mag_ref[...] / norm

        @pl.when(j >= lag)
        def _():
            c = chip_of(j - lag)
            need_ct(c)
            scale_sum(c)
            backward(c)

        @pl.when(j == 0)
        def _():
            handle(0)

        @pl.when(j < nz - 3)
        def _():
            handle(j + 1)

        @pl.when(j == nz - 2)
        def _():
            handle(last)

        @pl.when(j < held)
        def _():
            send_p(chip)

        return 0

    lax.fori_loop(0, nz, turn, 0)

    def finish_s(j, _):
        c = chip_of(j)
        need_ct(c)
        scale_sum(c)
        return 0

    lax.fori_loop(nz - lag, nz, finish_s, 0)
    SX[x] = jnp.sum(SACC[...], axis=0, keepdims=True)
    for d in range(1, nx):
        to_x(SX.at[x], SX.at[x], sx_s, sx_r, d).start()

    def finish_b(j, _):
        backward(chip_of(j))
        return 0

    lax.fori_loop(nz - lag, nz, finish_b, 0)
    for i in range(ny):
        H[i] = R[:, i * slab : (i + 1) * slab]
    for i in range(nx):
        BGS[i] = BG[:, i * part : (i + 1) * part]

    for d in range(1, nx):
        from_x(SX, sx_r, sx_s, d).wait_recv()
    sx = SX[0]
    for i in range(1, nx):
        sx = sx + SX[i]
    SY[y] = sx

    def to_y(src, slot, ssem, rsem, d):
        return copy(src, slot, ssem.at[d - 1], rsem.at[y], step(0, d, ny))

    def from_y(slots, rsem, ssem, d):
        src = lax.rem(y + d, ny)
        return copy(slots.at[src], slots.at[src], ssem.at[d - 1], rsem.at[src], step(0, d, ny))

    for d in range(1, ny):
        to_y(SY.at[y], SY.at[y], sy_s, sy_r, d).start()
    for d in range(1, nx):
        dst = lax.rem(x + d, nx)
        copy(BGS.at[dst], BX.at[x], bx_s.at[d - 1], bx_r.at[x], step(1, d, nx)).start()
    BX[x] = BGS[x]
    for d in range(1, ny):
        dst = lax.rem(y + d, ny)
        copy(H.at[dst], RY.at[y], ry_s.at[d - 1], ry_r.at[y], step(0, d, ny)).start()
    RY[y] = H[y]

    def send_held(j, _):
        send_p(chip_of(j))
        return 0

    lax.fori_loop(held, nz, send_held, 0)

    for d in range(1, nx):
        from_x(BX, bx_r, bx_s, d).wait_recv()
    bx = BX[0]
    for i in range(1, nx):
        bx = bx + BX[i]
    BY[y] = bx
    for d in range(1, ny):
        to_y(BY.at[y], BY.at[y], by_s, by_r, d).start()

    for d in range(1, ny):
        from_y(SY, sy_r, sy_s, d).wait_recv()
    s_all = SY[0]
    for i in range(1, ny):
        s_all = s_all + SY[i]
    norm = NORM[...]
    gmag_ref[...] = s_all / norm
    coef = -s_all * mag_ref[...] / (norm * norm * norm)
    scaled = (B[...].astype(F32) * coef).astype(BF16)
    cols = pl.ds(pl.multiple_of(y * slab, slab), slab)
    part_y = nt(scaled, W[cols, :]) + exact(nt(scaled, B[...]), A[:, cols].astype(F32))
    for d in range(1, ny):
        from_y(RY, ry_r, ry_s, d).wait_recv()
    for i in range(ny):
        part_y = part_y + RY[i]

    CX[0] = part_y[:, :lane]
    CX[1] = part_y[:, lane:]
    cross = copy(CX.at[1 - k], CX.at[2], cx_s.at[0], cx_r.at[0], partner)
    cross.start()
    cross.wait_recv()
    ZX[z] = CX[k] + CX[2]

    def to_z(d):
        return copy(ZX.at[z], ZX.at[z], zx_s.at[d - 1], zx_r.at[z], step(2, d, nz))

    for d in range(1, nz):
        to_z(d).start()

    for d in range(1, ny):
        from_y(BY, by_r, by_s, d).wait_recv()
    b_all = BY[0]
    for i in range(1, ny):
        b_all = b_all + BY[i]
    for d in range(1, nx):
        from_x(AX, ax_r, ax_s, d).wait_recv()
    a_all = AX[0]
    for i in range(1, nx):
        a_all = a_all + AX[i]

    for i in range(nx):

        @pl.when(x == i)
        def _():
            c = slice(i * part, (i + 1) * part)
            gb_ref[:, c] = b_all + a_all * coef[:, c]

    def gb_part(i):
        return gb_ref.at[:, pl.ds(pl.multiple_of(i * part, part), part)]

    for d in range(1, nx):
        copy(gb_part(x), gb_part(x), bo_s.at[d - 1], bo_r.at[x], step(1, d, nx)).start()

    for d in range(1, nx):
        src = lax.rem(x + d, nx)
        for loc in range(per):
            p_copy(x * per + loc, src, src).wait_recv()
    rest = pl.ds(pl.multiple_of(x * own, own), own)
    total = PF[rest, :]
    for d in range(1, nx):
        total = total + PR[lax.rem(x + d, nx)].astype(F32)
    proj_ref[...] = (total * SCALE[...]).astype(BF16)

    def from_z(d):
        src = lax.rem(z + d, nz)
        return copy(ZX.at[src], ZX.at[src], zx_s.at[d - 1], zx_r.at[src], step(2, d, nz))

    for d in range(1, nz):
        from_z(d).wait_recv()
    whole = ZX[0]
    for i in range(1, nz):
        whole = whole + ZX[i]

    def ifg_part(i, core):
        return ifg_ref.at[:, pl.ds(pl.multiple_of(i * slab + core * lane, lane), lane)]

    ifg_ref[:, pl.ds(pl.multiple_of(y * slab + k * lane, lane), lane)] = whole
    for d in range(1, ny):
        copy(ifg_part(y, k), ifg_part(y, k), yo_s.at[d - 1], yo_r.at[y], step(0, d, ny)).start()

    def core_copy(i, core):
        return copy(ifg_part(i, core), ifg_part(i, core), co_s.at[i], co_r.at[i], partner)

    core_copy(y, k).start()
    for d in range(1, ny):
        by = (d + 1) // 2 if d % 2 else -(d // 2)
        src = lax.rem(y + by + ny, ny)
        copy(ifg_part(src, k), ifg_part(src, k), yo_s.at[0], yo_r.at[src], step(0, 1, ny)).wait_recv()
        core_copy(src, k).start()
    for d in range(1, nx):
        src = lax.rem(x + d, nx)
        copy(gb_part(src), gb_part(src), bo_s.at[d - 1], bo_r.at[src], step(1, d, nx)).wait_recv()
    for i in range(ny):
        core_copy(i, 1 - k).wait_recv()

    def sent(src, ssem, dev):
        copy(src, src, ssem, ssem, dev).wait_send()

    for i in range(last + 1):
        sent(T.at[pl.ds(0, half)], zr_s.at[i], right)
        sent(T.at[pl.ds(0, half)], zl_s.at[i], left)
        sent(T.at[pl.ds(0, half)], dr_s.at[i], partner)
        sent(T.at[pl.ds(0, half)], dl_s.at[i], partner)
    sent(T.at[pl.ds(0, rows)], do_s.at[0], partner)
    for d in range(1, nx):
        dev = step(1, d, nx)
        for i in range(per):
            sent(CT.at[pl.ds(0, unit)], ct_s.at[(d - 1) * per + i], dev)
        sent(NX.at[0], nx_s.at[d - 1], dev)
        sent(AM.at[0], ax_s.at[d - 1], dev)
        sent(SX.at[0], sx_s.at[d - 1], dev)
        sent(BX.at[0], bx_s.at[d - 1], dev)
        sent(gb_part(0), bo_s.at[d - 1], dev)

    def sent_p(chip, _):
        @pl.when(chip // per != x)
        def _():
            p_copy(chip, x, chip // per).wait_send()

        return 0

    lax.fori_loop(0, nz, sent_p, 0)
    for d in range(1, ny):
        dev = step(0, d, ny)
        sent(SY.at[0], sy_s.at[d - 1], dev)
        sent(BY.at[0], by_s.at[d - 1], dev)
        sent(RY.at[0], ry_s.at[d - 1], dev)
        sent(ifg_part(0, 0), yo_s.at[d - 1], dev)
    sent(CX.at[0], cx_s.at[0], partner)
    for d in range(1, nz):
        sent(ZX.at[0], zx_s.at[d - 1], step(2, d, nz))
    for i in range(ny):
        sent(ifg_part(0, 0), co_s.at[i], partner)


def per_device(sizes, tokens, weight, a, b, magnitude, cotangent, lengths):
    ny, nx, nz = sizes
    rows, feats = tokens.shape
    rank, cols = b.shape
    group = rows * 2 * nz
    own = group // nx
    slab = feats // ny
    part = cols // nx
    per = nz // nx
    ring = nz - 1
    V = pltpu.VMEM
    S = lambda n: pltpu.SemaphoreType.DMA((n,))
    pairs = lambda n: [S(n), S(n)]
    outs = pl.pallas_call(
        functools.partial(kernel, sizes),
        out_shape=(
            jax.ShapeDtypeStruct((own, cols), BF16),
            jax.ShapeDtypeStruct((1, cols), F32),
            jax.ShapeDtypeStruct((rank, feats), F32),
            jax.ShapeDtypeStruct((rank, cols), F32),
        ),
        in_specs=[
            pl.BlockSpec(memory_space=pl.ANY),
            pl.BlockSpec(memory_space=pl.ANY),
            pl.BlockSpec(memory_space=pl.ANY),
            pl.BlockSpec(memory_space=pl.ANY),
            pl.BlockSpec(memory_space=pltpu.VMEM),
            pl.BlockSpec(memory_space=pl.ANY),
            pl.BlockSpec(memory_space=pltpu.SMEM),
        ],
        out_specs=[pl.BlockSpec(memory_space=pltpu.VMEM)] * 4,
        scratch_shapes=[
            V((group, feats), BF16),
            V((feats, cols), BF16),
            V((rank, feats), BF16),
            V((rank, cols), BF16),
            V((group, cols), BF16),
            V((group, 128), F32),
            V((group, cols), F32),
            V((group, cols), BF16),
            V((nx, own, cols), BF16),
            V((group, rank), BF16),
            V((nx, 1, cols), F32),
            V((nx, rank, part), F32),
            V((8, cols), F32),
            V((nx, 1, cols), F32),
            V((ny, 1, cols), F32),
            V((1, cols), F32),
            V((1, cols), F32),
            V((rank, cols), F32),
            V((nx, rank, part), F32),
            V((nx, rank, part), F32),
            V((ny, rank, part), F32),
            V((rank, feats), F32),
            V((ny, rank, slab), F32),
            V((ny, rank, slab), F32),
            V((3, rank, slab // 2), F32),
            V((nz, rank, slab // 2), F32),
            V((nx, rank, part), F32),
            S(5),
            *pairs(ring), *pairs(ring), *pairs(ring), *pairs(ring), *pairs(1),
            S((nx - 1) * per), S(nz),
            S(nz), S(nx * per),
            S(nx - 1), S(nx), S(nx - 1), S(nx), S(nx - 1), S(nx),
            S(ny - 1), S(ny),
            S(nx - 1), S(nx),
            S(ny - 1), S(ny),
            S(nx - 1), S(nx),
            S(ny - 1), S(ny),
            *pairs(1),
            S(nz - 1), S(nz),
            S(ny - 1), S(ny),
            *pairs(ny),
        ],
        compiler_params=pltpu.CompilerParams(
            collective_id=0, has_side_effects=True, vmem_limit_bytes=56 * 1024 * 1024
        ),
        name="lora_step",
    )(tokens, weight, a, b, magnitude.reshape(1, cols), cotangent, lengths)
    proj, gmag, ifg, gb = outs
    return proj, gmag.reshape(cols), ifg, gb


def solution(mesh):
    ny, nx = mesh.shape["dp"], mesh.shape["row"]
    nz = mesh.shape["col"] // 2
    split = Mesh(mesh.devices.reshape(ny, nx, nz, 2), AXES)
    return jax.shard_map(
        functools.partial(per_device, (ny, nx, nz)),
        mesh=split,
        in_specs=(
            P(("dp", "z", "core"), "row"),
            P("row", COL),
            P(None, "row"),
            P(None, COL),
            P(COL),
            P(("dp", "row"), COL),
            P("dp", None),
        ),
        out_specs=(P(("dp", "row"), COL), P(COL), P(None, "row"), P(None, COL)),
        check_vma=False,
    )
```

```python
import functools

import jax
import jax.numpy as jnp
from jax import lax
from jax.experimental import pallas as pl
from jax.experimental.pallas import tpu as pltpu
from jax.sharding import Mesh
from jax.sharding import PartitionSpec as P

AXES = ("dp", "row", "z", "core")
COL = ("z", "core")
EPS = 1e-06
F32 = jnp.float32
BF16 = jnp.bfloat16
HIGHEST = lax.Precision.HIGHEST
PIECES = 4
EARLY = 6


def nn(a, b):
    return lax.dot_general(a, b, (((1,), (0,)), ((), ())), preferred_element_type=F32)


def nt(a, b):
    return lax.dot_general(a, b, (((1,), (1,)), ((), ())), preferred_element_type=F32)


def tn(a, b):
    return lax.dot_general(a, b, (((0,), (0,)), ((), ())), preferred_element_type=F32)


def exact(a, b):
    return lax.dot_general(
        a, b, (((1,), (0,)), ((), ())), preferred_element_type=F32, precision=HIGHEST
    )


def far_first(n):
    return sorted(range(1, n), key=lambda d: -min(d, n - d))


def fold(a):
    return jnp.sum(a.reshape(a.shape[0] // 8, 8, a.shape[1]), axis=0)


def kernel(
    sizes,
    tok_hbm, w_hbm, a_hbm, b_hbm, mag_hbm, ct_hbm, lens_hbm,
    proj_ref, gmag_ref, ifg_ref, gb_ref,
    T, W, A, B, CT, WT, PF, PS, PR, DB,
    NX, AX, SACC, SX, SY, SCALE, NORM, BG, BGS, BX, BY, R, RY, H, RL, HL, CX, ZX, AM, MAG, LENS,
    load_sem, zr_s, zr_r, zl_s, zl_r, dr_s, dr_r, dl_s, dl_r, do_s, do_r,
    ct_s, ct_r, p_s, p_r, nx_s, nx_r, ax_s, ax_r, sx_s, sx_r, sy_s, sy_r,
    bx_s, bx_r, by_s, by_r, bo_s, bo_r, ry_s, ry_r, cx_s, cx_r, zx_s, zx_r,
    yo_s, yo_r, co_s, co_r, rl_s, rl_r, wave,
):
    ny, nx, nz = sizes
    y, x, z, k = (lax.axis_index(a) for a in AXES)
    rows = tok_hbm.shape[0]
    piece = rows // PIECES
    unit = 2 * rows
    own = nz // nx * unit
    per = nz // nx
    slab = T.shape[1] // ny
    lane = slab // 2
    part = W.shape[1] // nx

    def at(axis, index):
        return tuple(index if i == axis else v for i, v in enumerate((y, x, z, k)))

    def step(axis, by, n):
        return at(axis, lax.rem((y, x, z)[axis] + by + n, n))

    partner = (y, x, z, 1 - k)
    right = step(2, 1, nz)
    left = step(2, -1, nz)

    def copy(src, dst, ssem, rsem, dev):
        return pltpu.make_async_remote_copy(
            src_ref=src, dst_ref=dst, send_sem=ssem, recv_sem=rsem,
            device_id=dev, device_id_type=pl.DeviceIdType.MESH,
        )

    barrier = pltpu.get_barrier_semaphore()
    near = [partner] + [step(axis, d, n) for axis, n in ((2, nz), (1, nx), (0, ny)) for d in (1, -1)]

    def signal(sem, dev):
        pl.semaphore_signal(sem, inc=1, device_id=dev, device_id_type=pl.DeviceIdType.MESH)

    for dev in near:
        signal(barrier, dev)

    def token_rows(chip, core, h, n):
        return pl.ds(pl.multiple_of(chip * unit + core * rows + h * piece, piece), n)

    mine = token_rows(z, k, 0, rows)
    owned = pl.ds(pl.multiple_of(x * own, own), own)
    loads = [
        pltpu.make_async_copy(tok_hbm, T.at[mine], load_sem.at[0]),
        pltpu.make_async_copy(ct_hbm, CT.at[owned], load_sem.at[1]),
        pltpu.make_async_copy(a_hbm, A, load_sem.at[2]),
        pltpu.make_async_copy(b_hbm, B, load_sem.at[3]),
        pltpu.make_async_copy(w_hbm, W, load_sem.at[4]),
        pltpu.make_async_copy(mag_hbm, MAG, load_sem.at[5]),
        pltpu.make_async_copy(lens_hbm, LENS, load_sem.at[6]),
    ]
    for c in loads:
        c.start()

    seqs = LENS.shape[1]

    def weigh(i, _):
        pos = lax.broadcasted_iota(jnp.int32, (unit, 128), 0) + i * unit
        total = jnp.zeros((unit, 128), F32)
        start = jnp.int32(0)
        for s in range(seqs):
            length = LENS[0, s]
            end = start + length
            inverse = 1.0 / jnp.full((1, 128), length, jnp.int32).astype(F32)
            total += jnp.where((pos >= start) & (pos < end), inverse, 0.0)
            start = end
        WT[pl.ds(pl.multiple_of(i * unit, unit), unit), :] = total
        return 0

    loads[0].wait()
    pl.semaphore_wait(barrier, len(near))

    def ring(right_way, src_chip, h, idx):
        r = token_rows(src_chip, k, h, piece)
        if right_way:
            return copy(T.at[r], T.at[r], zr_s.at[idx], zr_r.at[idx], right)
        return copy(T.at[r], T.at[r], zl_s.at[idx], zl_r.at[idx], left)

    def across(right_way, src_chip, core, h, idx):
        r = token_rows(src_chip, core, h, piece)
        if right_way:
            return copy(T.at[r], T.at[r], dr_s.at[idx], dr_r.at[idx], partner)
        return copy(T.at[r], T.at[r], dl_s.at[idx], dl_r.at[idx], partner)

    def across_own(core):
        r = token_rows(z, core, 0, rows)
        return copy(T.at[r], T.at[r], do_s.at[0], do_r.at[0], partner)

    full = (nz // 2 - 1) * PIECES
    pieces = full + PIECES // 2
    for h in range(PIECES):
        ring(True, z, h, h).start()
        ring(False, z, h, h).start()
    across_own(k).start()

    levels = {0: ny // 2 - 1, 1: nx // 2 - 1, 2: nz // 2 - 1}
    base = {1: 0, 0: levels[1], 2: levels[1] + levels[0]}

    def tell(axis, level):
        for d in (1, -1):
            signal(wave.at[base[axis] + level], step(axis, d, (ny, nx, nz)[axis]))

    def hear(axis, level):
        pl.semaphore_wait(wave.at[base[axis] + level], 2)

    tell(1, 0)
    tell(2, 0)
    loads[6].wait()
    lax.fori_loop(0, nz, weigh, 0)
    for level in range(levels[1]):
        hear(1, level)
        if level + 1 < levels[1]:
            tell(1, level + 1)
    tell(0, 0)

    def spread_word(level):
        for axis in (0, 2):
            if level < levels[axis]:
                hear(axis, level)
            if level + 1 < levels[axis]:
                tell(axis, level + 1)

    def chip_of(j):
        s = (j + 1) // 2
        return lax.rem(z + nz + jnp.where(lax.rem(j, 2) == 1, -s, s), nz)

    def unit_rows(chip):
        return pl.ds(pl.multiple_of(chip * unit, unit), unit)

    def turn_of(chip):
        d = lax.rem(chip - z + nz, nz)
        return jnp.where(d < nz // 2, 2 * d, 2 * (nz - d) - 1)

    ahead = jnp.where(turn_of(x * per) < turn_of(x * per + 1), 0, 1)
    strip = unit // 2
    strips = per * 2 * (nx - 1)

    def ct_copy(loc, part_of, dx, src_x):
        r = pl.ds(pl.multiple_of((src_x * per + loc) * unit + part_of * strip, strip), strip)
        d = lax.rem(dx - src_x + nx, nx)
        return copy(
            CT.at[r], CT.at[r], ct_s.at[(d - 1) * 2 * per + 2 * loc + part_of],
            ct_r.at[src_x * 2 * per + 2 * loc + part_of], at(1, dx),
        )

    def send_ct(n, _):
        u = n // (strips // per)
        loc = jnp.where(u == 0, ahead, 1 - ahead)
        m = lax.rem(n, strips // per)
        ct_copy(loc, m // (nx - 1), lax.rem(x + 1 + lax.rem(m, nx - 1), nx), x).start()
        return 0

    loads[1].wait()
    lax.fori_loop(0, EARLY, send_ct, 0)

    for c in loads[2:6]:
        c.wait()
    chunk = slab

    def norm_part(i, acc):
        c = pl.ds(pl.multiple_of(i * chunk, chunk), chunk)
        m = W[c, :].astype(F32) + tn(A[:, c], B[...])
        return acc + fold(m * m)

    acc = lax.fori_loop(0, ny, norm_part, jnp.zeros((8, W.shape[1]), F32), unroll=4)
    NX[x] = jnp.sum(acc, axis=0, keepdims=True)

    def to_x(src, slot, ssem, rsem, d):
        return copy(src, slot, ssem.at[d - 1], rsem.at[x], step(1, d, nx))

    def from_x(slots, rsem, ssem, d):
        src = lax.rem(x + d, nx)
        return copy(slots.at[src], slots.at[src], ssem.at[d - 1], rsem.at[src], step(1, d, nx))

    for d in range(1, nx):
        to_x(NX.at[x], NX.at[x], nx_s, nx_r, d).start()

    SACC[...] = jnp.zeros_like(SACC)
    BG[...] = jnp.zeros_like(BG)
    R[...] = jnp.zeros_like(R)

    def low_rank():
        am = nn(A[...], W[...]) + exact(nt(A[...], A[...]), B[...].astype(F32))
        for i in range(nx):
            AM[i] = am[:, i * part : (i + 1) * part]
        AX[x] = AM[x]
        for d in range(1, nx):
            dst = lax.rem(x + d, nx)
            copy(AM.at[dst], AX.at[x], ax_s.at[d - 1], ax_r.at[x], step(1, d, nx)).start()

    def project(chip):
        r = unit_rows(chip)
        t = T[r, :]
        down = nt(t, A[...]).astype(BF16)
        p = nn(t, W[...]) + nn(down, B[...])
        DB[r, :] = down
        PF[r, :] = p
        PS[r, :] = p.astype(BF16)

    def need_ct(chip):
        @pl.when(chip // per != x)
        def _():
            for h in range(2):
                ct_copy(lax.rem(chip, per), h, x, chip // per).wait_recv()

    def weighted(chip):
        r = unit_rows(chip)
        w = WT[r, :]
        return CT[r, :].astype(F32) * jnp.concatenate([w] * (W.shape[1] // 128), axis=1)

    def scale_sum(chip):
        SACC[...] += fold(weighted(chip) * PF[unit_rows(chip), :])

    def backward(chip):
        r = unit_rows(chip)
        gp = (weighted(chip) * SCALE[...]).astype(BF16)
        BG[...] += tn(DB[r, :], gp)
        back = nt(B[...], gp)
        high = back.astype(BF16)
        low = (back - high.astype(F32)).astype(BF16)
        both = nn(jnp.concatenate([high, low], axis=0), T[r, :])
        R[...] += both[: back.shape[0]] + both[back.shape[0] :]

    def p_copy(chip, src, dst):
        loc = lax.rem(chip, per)
        r = pl.ds(pl.multiple_of(loc * unit, unit), unit)
        return copy(
            PS.at[unit_rows(chip)], PR.at[src, r], p_s.at[chip], p_r.at[src * per + loc], at(1, dst)
        )

    def send_p(chip):
        @pl.when(chip // per != x)
        def _():
            p_copy(chip, x, chip // per).start()

    def handle(i):
        s = i // PIECES + 1
        h = lax.rem(i, PIECES)
        far = i >= full
        other = PIECES // 2
        hl = jnp.where(far, h + other, h)
        fr = lax.rem(z - s + nz, nz)
        fl = lax.rem(z + s, nz)
        third = i >= full - PIECES
        ring(True, fr, h, i).wait_recv()

        @pl.when((i < full - PIECES) | (third & (h < other) & (i < full)))
        def _():
            ring(True, fr, h, i + PIECES).start()

        across(True, fr, k, h, i).start()
        ring(False, fl, hl, i).wait_recv()

        @pl.when((i < full - PIECES) | (third & (h >= other) & (i < full)))
        def _():
            ring(False, fl, hl, jnp.where(third, i + PIECES - other, i + PIECES)).start()

        across(False, fl, k, hl, i).start()

        @pl.when(i + EARLY < strips)
        def _():
            send_ct(i + EARLY, 0)

    def need_tokens(j):
        chip = chip_of(j)

        @pl.when(j == 0)
        def _():
            across_own(1 - k).wait_recv()

        @pl.when((lax.rem(j, 2) == 1) & (j < nz - 1))
        def _():
            for h in range(PIECES):
                across(True, chip, 1 - k, h, (j - 1) // 2 * PIECES + h).wait_recv()

        @pl.when((lax.rem(j, 2) == 0) & (j > 0))
        def _():
            for h in range(PIECES):
                across(False, chip, 1 - k, h, (j - 2) // 2 * PIECES + h).wait_recv()

        @pl.when(j == nz - 1)
        def _():
            for h in range(PIECES // 2):
                across(True, chip, 1 - k, h, full + h).wait_recv()
                across(False, chip, 1 - k, h + PIECES // 2, full + h).wait_recv()

    def handle_range(low, high):
        def one(i, _):
            handle(i)
            return 0

        lax.fori_loop(low, high, one, 0)

    held = nz - 3

    def settle(j, _):
        c = chip_of(j)
        need_ct(c)
        scale_sum(c)
        backward(c)
        return 0

    def turn(j, _):
        chip = chip_of(j)
        need_tokens(j)
        project(chip)

        @pl.when(j == 1)
        def _():
            for d in range(1, nx):
                from_x(NX, nx_r, nx_s, d).wait_recv()
            sq = NX[0]
            for i in range(1, nx):
                sq = sq + NX[i]
            norm = jnp.sqrt(sq + EPS)
            NORM[...] = norm
            SCALE[...] = MAG[...] / norm

        mid = j < nz - 3
        inner = jnp.where(mid, PIECES // 2 * (j + 1), jnp.where(j == nz - 3, full, pieces - 1))
        outer = jnp.where(mid, inner + PIECES // 2, jnp.where(j == nz - 3, pieces - 1, pieces))
        handle_range(jnp.where(j == 0, 0, inner), jnp.where(j == 0, PIECES, jnp.where(j == nz - 1, inner, outer)))

        @pl.when(j == 0)
        def _():
            low_rank()

        for level in range(max(levels.values())):

            @pl.when(j == level)
            def _():
                spread_word(level)

        @pl.when(j < held)
        def _():
            send_p(chip)

        low = jnp.where(j == nz - 2, nz - 5, j - 2)
        high = jnp.where(j == nz - 2, nz - 2, jnp.where((j >= 2) & (j < nz - 3), j - 1, low))
        lax.fori_loop(low, high, settle, 0)

        @pl.when(j == nz - 2)
        def _():
            for i in range(ny):
                H[i] = R[:, i * slab : (i + 1) * slab]
            R[...] = jnp.zeros_like(R)
            RY[y] = H[y]
            for d in far_first(ny):
                dst = lax.rem(y + d, ny)
                copy(H.at[dst], RY.at[y], ry_s.at[d - 1], ry_r.at[y], step(0, d, ny)).start()

        return 0

    lax.fori_loop(0, nz, turn, 0)

    def finish_s(j, _):
        c = chip_of(j)
        need_ct(c)
        scale_sum(c)
        return 0

    lax.fori_loop(nz - 2, nz, finish_s, 0)
    SX[x] = jnp.sum(SACC[...], axis=0, keepdims=True)
    for d in far_first(nx):
        to_x(SX.at[x], SX.at[x], sx_s, sx_r, d).start()

    def finish_b(j, _):
        backward(chip_of(j))
        return 0

    lax.fori_loop(nz - 2, nz, finish_b, 0)
    for i in range(ny):
        HL[i] = R[:, i * slab : (i + 1) * slab].astype(BF16)
    RL[y] = HL[y]
    for d in far_first(ny):
        dst = lax.rem(y + d, ny)
        copy(HL.at[dst], RL.at[y], rl_s.at[d - 1], rl_r.at[y], step(0, d, ny)).start()
    for i in range(nx):
        BGS[i] = BG[:, i * part : (i + 1) * part]
    BX[x] = BGS[x]

    for d in range(1, nx):
        from_x(SX, sx_r, sx_s, d).wait_recv()
    sx = SX[0]
    for i in range(1, nx):
        sx = sx + SX[i]
    SY[y] = sx

    def to_y(src, slot, ssem, rsem, d):
        return copy(src, slot, ssem.at[d - 1], rsem.at[y], step(0, d, ny))

    def from_y(slots, rsem, ssem, d):
        src = lax.rem(y + d, ny)
        return copy(slots.at[src], slots.at[src], ssem.at[d - 1], rsem.at[src], step(0, d, ny))

    for d in far_first(ny):
        to_y(SY.at[y], SY.at[y], sy_s, sy_r, d).start()
    for d in range(1, nx):
        dst = lax.rem(x + d, nx)
        copy(BGS.at[dst], BX.at[x], bx_s.at[d - 1], bx_r.at[x], step(1, d, nx)).start()

    def send_held(j, _):
        send_p(chip_of(j))
        return 0

    lax.fori_loop(held, nz, send_held, 0)

    for d in range(1, ny):
        from_y(RY, ry_r, ry_s, d).wait_recv()
    row_part = RY[0]
    for i in range(1, ny):
        row_part = row_part + RY[i]
    norm = NORM[...]
    inverse = 1.0 / norm
    slope = -MAG[...] * (inverse * inverse * inverse)

    for d in range(1, ny):
        from_y(SY, sy_r, sy_s, d).wait_recv()
    s_all = SY[0]
    for i in range(1, ny):
        s_all = s_all + SY[i]
    coef = s_all * slope
    scaled = (B[...].astype(F32) * coef).astype(BF16)
    cols = pl.ds(pl.multiple_of(y * slab, slab), slab)
    part_y = nt(scaled, W[cols, :]) + exact(nt(scaled, B[...]), A[:, cols].astype(F32))
    for d in range(1, ny):
        from_y(RL, rl_r, rl_s, d).wait_recv()
    for i in range(ny):
        row_part = row_part + RL[i].astype(F32)
    part_y = part_y + row_part

    CX[0] = part_y[:, :lane]
    CX[1] = part_y[:, lane:]
    cross = copy(CX.at[1 - k], CX.at[2], cx_s.at[0], cx_r.at[0], partner)
    cross.start()
    cross.wait_recv()
    ZX[z] = CX[k] + CX[2]

    def to_z(d):
        return copy(ZX.at[z], ZX.at[z], zx_s.at[d - 1], zx_r.at[z], step(2, d, nz))

    for d in far_first(nz):
        to_z(d).start()
    gmag_ref[...] = s_all * inverse

    for d in range(1, nx):
        from_x(BX, bx_r, bx_s, d).wait_recv()
    bx = BX[0]
    for i in range(1, nx):
        bx = bx + BX[i]
    BY[y] = bx
    for d in far_first(ny):
        to_y(BY.at[y], BY.at[y], by_s, by_r, d).start()
    for d in range(1, nx):
        from_x(AX, ax_r, ax_s, d).wait_recv()
    a_all = AX[0]
    for i in range(1, nx):
        a_all = a_all + AX[i]

    for d in range(1, nx):
        src = lax.rem(x + d, nx)
        for loc in range(per):
            p_copy(x * per + loc, src, src).wait_recv()
    rest = pl.ds(pl.multiple_of(x * own, own), own)
    total = PF[rest, :]
    for d in range(1, nx):
        total = total + PR[lax.rem(x + d, nx)].astype(F32)
    proj_ref[...] = (total * SCALE[...]).astype(BF16)

    def from_z(d):
        src = lax.rem(z + d, nz)
        return copy(ZX.at[src], ZX.at[src], zx_s.at[d - 1], zx_r.at[src], step(2, d, nz))

    for d in range(1, nz):
        from_z(d).wait_recv()
    whole = ZX[0]
    for i in range(1, nz):
        whole = whole + ZX[i]

    def ifg_part(i, core):
        return ifg_ref.at[:, pl.ds(pl.multiple_of(i * slab + core * lane, lane), lane)]

    ifg_ref[:, pl.ds(pl.multiple_of(y * slab + k * lane, lane), lane)] = whole
    for d in far_first(ny):
        copy(ifg_part(y, k), ifg_part(y, k), yo_s.at[d - 1], yo_r.at[y], step(0, d, ny)).start()

    def core_copy(i, core):
        return copy(ifg_part(i, core), ifg_part(i, core), co_s.at[i], co_r.at[i], partner)

    core_copy(y, k).start()

    for d in range(1, ny):
        from_y(BY, by_r, by_s, d).wait_recv()
    b_all = BY[0]
    for i in range(1, ny):
        b_all = b_all + BY[i]

    for i in range(nx):

        @pl.when(x == i)
        def _():
            c = slice(i * part, (i + 1) * part)
            gb_ref[:, c] = b_all + a_all * coef[:, c]

    def gb_part(i):
        return gb_ref.at[:, pl.ds(pl.multiple_of(i * part, part), part)]

    for d in range(1, nx):
        copy(gb_part(x), gb_part(x), bo_s.at[d - 1], bo_r.at[x], step(1, d, nx)).start()

    for d in range(1, ny):
        by = (d + 1) // 2 if d % 2 else -(d // 2)
        src = lax.rem(y + by + ny, ny)
        copy(ifg_part(src, k), ifg_part(src, k), yo_s.at[0], yo_r.at[src], step(0, 1, ny)).wait_recv()
        core_copy(src, k).start()
    for d in range(1, nx):
        src = lax.rem(x + d, nx)
        copy(gb_part(src), gb_part(src), bo_s.at[d - 1], bo_r.at[src], step(1, d, nx)).wait_recv()
    for i in range(ny):
        core_copy(i, 1 - k).wait_recv()

    def sent(src, ssem, dev):
        copy(src, src, ssem, ssem, dev).wait_send()

    for i in range(pieces):
        sent(T.at[pl.ds(0, piece)], zr_s.at[i], right)
        sent(T.at[pl.ds(0, piece)], zl_s.at[i], left)
        sent(T.at[pl.ds(0, piece)], dr_s.at[i], partner)
        sent(T.at[pl.ds(0, piece)], dl_s.at[i], partner)
    sent(T.at[pl.ds(0, rows)], do_s.at[0], partner)
    for d in range(1, nx):
        dev = step(1, d, nx)
        for i in range(2 * per):
            sent(CT.at[pl.ds(0, strip)], ct_s.at[(d - 1) * 2 * per + i], dev)
        sent(NX.at[0], nx_s.at[d - 1], dev)
        sent(AM.at[0], ax_s.at[d - 1], dev)
        sent(SX.at[0], sx_s.at[d - 1], dev)
        sent(BX.at[0], bx_s.at[d - 1], dev)
        sent(gb_part(0), bo_s.at[d - 1], dev)

    def sent_p(chip, _):
        @pl.when(chip // per != x)
        def _():
            p_copy(chip, x, chip // per).wait_send()

        return 0

    lax.fori_loop(0, nz, sent_p, 0)
    for d in range(1, ny):
        dev = step(0, d, ny)
        sent(SY.at[0], sy_s.at[d - 1], dev)
        sent(BY.at[0], by_s.at[d - 1], dev)
        sent(RY.at[0], ry_s.at[d - 1], dev)
        sent(RL.at[0], rl_s.at[d - 1], dev)
        sent(ifg_part(0, 0), yo_s.at[d - 1], dev)
    sent(CX.at[0], cx_s.at[0], partner)
    for d in range(1, nz):
        sent(ZX.at[0], zx_s.at[d - 1], step(2, d, nz))
    for i in range(ny):
        sent(ifg_part(0, 0), co_s.at[i], partner)


def put_out(*refs):
    *pairs, sem = refs
    copies = [pltpu.make_async_copy(pairs[i], pairs[i + 4], sem.at[i]) for i in range(4)]
    for c in copies:
        c.start()
    for c in copies:
        c.wait()


def per_device(sizes, tokens, weight, a, b, magnitude, cotangent, lengths):
    ny, nx, nz = sizes
    rows, feats = tokens.shape
    rank, cols = b.shape
    group = rows * 2 * nz
    own = group // nx
    slab = feats // ny
    part = cols // nx
    per = nz // nx
    ring = (nz // 2 - 1) * PIECES + PIECES // 2
    words = ny // 2 + nx // 2 + nz // 2 - 3
    V = pltpu.VMEM
    S = lambda n: pltpu.SemaphoreType.DMA((n,))
    pairs = lambda n: [S(n), S(n)]
    outs = pl.pallas_call(
        functools.partial(kernel, sizes),
        out_shape=(
            V((own, cols), BF16),
            V((1, cols), F32),
            V((rank, feats), F32),
            V((rank, cols), F32),
        ),
        in_specs=[pl.BlockSpec(memory_space=pl.ANY)] * 7,
        out_specs=[pl.BlockSpec(memory_space=pltpu.VMEM)] * 4,
        scratch_shapes=[
            V((group, feats), BF16),
            V((feats, cols), BF16),
            V((rank, feats), BF16),
            V((rank, cols), BF16),
            V((group, cols), BF16),
            V((group, 128), F32),
            V((group, cols), F32),
            V((group, cols), BF16),
            V((nx, own, cols), BF16),
            V((group, rank), BF16),
            V((nx, 1, cols), F32),
            V((nx, rank, part), F32),
            V((8, cols), F32),
            V((nx, 1, cols), F32),
            V((ny, 1, cols), F32),
            V((1, cols), F32),
            V((1, cols), F32),
            V((rank, cols), F32),
            V((nx, rank, part), F32),
            V((nx, rank, part), F32),
            V((ny, rank, part), F32),
            V((rank, feats), F32),
            V((ny, rank, slab), F32),
            V((ny, rank, slab), F32),
            V((ny, rank, slab), BF16),
            V((ny, rank, slab), BF16),
            V((3, rank, slab // 2), F32),
            V((nz, rank, slab // 2), F32),
            V((nx, rank, part), F32),
            V((1, cols), F32),
            pltpu.SMEM(lengths.shape, jnp.int32),
            S(7),
            *pairs(ring), *pairs(ring), *pairs(ring), *pairs(ring), *pairs(1),
            S((nx - 1) * 2 * per), S(2 * nz),
            S(nz), S(nx * per),
            S(nx - 1), S(nx), S(nx - 1), S(nx), S(nx - 1), S(nx),
            S(ny - 1), S(ny),
            S(nx - 1), S(nx),
            S(ny - 1), S(ny),
            S(nx - 1), S(nx),
            S(ny - 1), S(ny),
            *pairs(1),
            S(nz - 1), S(nz),
            S(ny - 1), S(ny),
            *pairs(ny),
            S(ny - 1), S(ny),
            pltpu.SemaphoreType.REGULAR((words,)),
        ],
        compiler_params=pltpu.CompilerParams(
            collective_id=0, has_side_effects=True, vmem_limit_bytes=56 * 1024 * 1024
        ),
        name="lora_step",
    )(tokens, weight, a, b, magnitude.reshape(1, cols), cotangent, lengths)
    whole = [jax.ShapeDtypeStruct(o.shape, o.dtype) for o in outs]
    proj, gmag, ifg, gb = pl.pallas_call(
        put_out,
        out_shape=whole,
        in_specs=[pl.BlockSpec(memory_space=pltpu.VMEM)] * 4,
        out_specs=[pl.BlockSpec(memory_space=pl.ANY)] * 4,
        scratch_shapes=[S(4)],
        compiler_params=pltpu.CompilerParams(vmem_limit_bytes=1024 * 1024),
        name="put_out",
    )(*outs)
    return proj, gmag.reshape(cols), ifg, gb


def solution(mesh):
    ny, nx = mesh.shape["dp"], mesh.shape["row"]
    nz = mesh.shape["col"] // 2
    split = Mesh(mesh.devices.reshape(ny, nx, nz, 2), AXES)
    return jax.shard_map(
        functools.partial(per_device, (ny, nx, nz)),
        mesh=split,
        in_specs=(
            P(("dp", "z", "core"), "row"),
            P("row", COL),
            P(None, "row"),
            P(None, COL),
            P(COL),
            P(("dp", "row"), COL),
            P("dp", None),
        ),
        out_specs=(P(("dp", "row"), COL), P(COL), P(None, "row"), P(None, COL)),
        check_vma=False,
    )
```

```python
import functools

import jax
import jax.numpy as jnp
from jax import lax
from jax.experimental import pallas as pl
from jax.experimental.pallas import tpu as pltpu
from jax.sharding import Mesh
from jax.sharding import PartitionSpec as P

AXES = ("dp", "row", "z", "core")
COL = ("z", "core")
EPS = 1e-06
F32 = jnp.float32
BF16 = jnp.bfloat16
HIGHEST = lax.Precision.HIGHEST
HELD = 5
PIECES = 4
EARLY = 6


LEAVE = ("zr", "zl", "d", "own", "ct", "p", "nx", "ax", "s", "bx", "by", "bo", "ry", "rl", "zx", "if")
ENTER = ("p", "nx", "ax", "s", "bx", "by", "bo", "ry", "rl", "zx", "if")


def nn(a, b):
    return lax.dot_general(a, b, (((1,), (0,)), ((), ())), preferred_element_type=F32)


def nt(a, b):
    return lax.dot_general(a, b, (((1,), (1,)), ((), ())), preferred_element_type=F32)


def tn(a, b):
    return lax.dot_general(a, b, (((0,), (0,)), ((), ())), preferred_element_type=F32)


def exact(a, b):
    return lax.dot_general(
        a, b, (((1,), (0,)), ((), ())), preferred_element_type=F32, precision=HIGHEST
    )


def far_first(n):
    return sorted(range(1, n), key=lambda d: -min(d, n - d))


def fold(a):
    return jnp.sum(a.reshape(a.shape[0] // 8, 8, a.shape[1]), axis=0)


def kernel(
    sizes,
    tok_hbm, w_hbm, a_hbm, b_hbm, mag_hbm, ct_hbm, lens_hbm,
    proj_ref, gmag_ref, ifg_ref, gb_ref,
    T, W, A, B, CT, WT, PF, PS, PR, PV, DB,
    NX, AX, SACC, SS, SCALE, NORM, BG, BGS, BX, BY, R, RY, H, RL, HL, CX, ZX, IF, AM, WX, MAG, LENS,
    load_sem, zr_r, zl_r, d_r, ct_r, pv_r, out_sem, in_sem, wave,
):
    ny, nx, nz = sizes
    y, x, z, k = (lax.axis_index(a) for a in AXES)
    rows = tok_hbm.shape[0]
    piece = rows // PIECES
    unit = 2 * rows
    own = nz // nx * unit
    per = nz // nx
    slab = T.shape[1] // ny
    lane = slab // 2
    part = W.shape[1] // nx

    def at(axis, index):
        return tuple(index if i == axis else v for i, v in enumerate((y, x, z, k)))

    def step(axis, by, n):
        return at(axis, lax.rem((y, x, z)[axis] + by + n, n))

    def leave(name):
        return out_sem.at[LEAVE.index(name)]

    def enter(name):
        return in_sem.at[ENTER.index(name)]

    partner = (y, x, z, 1 - k)
    right = step(2, 1, nz)
    left = step(2, -1, nz)

    def copy(src, dst, ssem, rsem, dev):
        return pltpu.make_async_remote_copy(
            src_ref=src, dst_ref=dst, send_sem=ssem, recv_sem=rsem,
            device_id=dev, device_id_type=pl.DeviceIdType.MESH,
        )

    def arrived(sem, ref):
        copy(ref, ref, sem, sem, partner).wait_recv()

    barrier = pltpu.get_barrier_semaphore()
    near = [partner] + [step(axis, d, n) for axis, n in ((2, nz), (1, nx), (0, ny)) for d in (1, -1)]

    def signal(sem, dev):
        pl.semaphore_signal(sem, inc=1, device_id=dev, device_id_type=pl.DeviceIdType.MESH)

    for dev in near:
        signal(barrier, dev)

    def token_rows(chip, core, h, n):
        return pl.ds(pl.multiple_of(chip * unit + core * rows + h * piece, piece), n)

    mine = token_rows(z, k, 0, rows)
    owned = pl.ds(pl.multiple_of(x * own, own), own)
    loads = [
        pltpu.make_async_copy(tok_hbm, T.at[mine], load_sem.at[0]),
        pltpu.make_async_copy(ct_hbm, CT.at[owned], load_sem.at[1]),
        pltpu.make_async_copy(a_hbm, A, load_sem.at[2]),
        pltpu.make_async_copy(b_hbm, B, load_sem.at[3]),
        pltpu.make_async_copy(w_hbm, W, load_sem.at[4]),
        pltpu.make_async_copy(mag_hbm, MAG, load_sem.at[5]),
        pltpu.make_async_copy(lens_hbm, LENS, load_sem.at[6]),
    ]
    for c in loads:
        c.start()

    seqs = LENS.shape[1]

    def weigh(i, _):
        pos = lax.broadcasted_iota(jnp.int32, (unit, 128), 0) + i * unit
        total = jnp.zeros((unit, 128), F32)
        start = jnp.int32(0)
        for s in range(seqs):
            length = LENS[0, s]
            end = start + length
            inverse = 1.0 / jnp.full((1, 128), length, jnp.int32).astype(F32)
            total += jnp.where((pos >= start) & (pos < end), inverse, 0.0)
            start = end
        WT[pl.ds(pl.multiple_of(i * unit, unit), unit), :] = total
        return 0

    loads[0].wait()
    pl.semaphore_wait(barrier, len(near))

    def ring(right_way, src_chip, h, idx):
        r = token_rows(src_chip, k, h, piece)
        if right_way:
            return copy(T.at[r], T.at[r], leave("zr"), zr_r.at[idx], right)
        return copy(T.at[r], T.at[r], leave("zl"), zl_r.at[idx], left)

    def across(src_chip, h, j):
        r = token_rows(src_chip, k, h, piece)
        return copy(T.at[r], T.at[r], leave("d"), d_r.at[j], partner)

    full = (nz // 2 - 1) * PIECES
    pieces = full + PIECES // 2
    for h in range(PIECES):
        ring(True, z, h, h).start()
        ring(False, z, h, h).start()
    copy(T.at[mine], T.at[mine], leave("own"), d_r.at[0], partner).start()

    levels = {0: ny // 2, 1: nx // 2 - 1, 2: nz // 2 - 1}
    base = {1: 0, 0: levels[1], 2: levels[1] + levels[0]}

    def tell(axis, level):
        for d in (1, -1):
            signal(wave.at[base[axis] + level], step(axis, d, (ny, nx, nz)[axis]))

    def hear(axis, level):
        pl.semaphore_wait(wave.at[base[axis] + level], 2)

    tell(1, 0)
    tell(2, 0)
    loads[6].wait()
    lax.fori_loop(0, nz, weigh, 0)
    def spread_word(level):
        for axis in (0, 2):
            if level < levels[axis]:
                hear(axis, level)
            if level + 1 < levels[axis]:
                tell(axis, level + 1)

    def chip_of(j):
        s = (j + 1) // 2
        return lax.rem(z + nz + jnp.where(lax.rem(j, 2) == 1, -s, s), nz)

    def unit_rows(chip):
        return pl.ds(pl.multiple_of(chip * unit, unit), unit)

    def turn_of(chip):
        d = lax.rem(chip - z + nz, nz)
        return jnp.where(d < nz // 2, 2 * d, 2 * (nz - d) - 1)

    ahead = jnp.where(turn_of(x * per) < turn_of(x * per + 1), 0, 1)
    strip = unit // 2
    strips = per * 2 * (nx - 1)

    def ct_copy(loc, part_of, dx, src_x):
        r = pl.ds(pl.multiple_of((src_x * per + loc) * unit + part_of * strip, strip), strip)
        d = lax.rem(dx - src_x + nx, nx)
        return copy(CT.at[r], CT.at[r], leave("ct"), ct_r.at[src_x * per + loc], at(1, dx))

    def send_ct(n, _):
        u = n // (strips // per)
        loc = jnp.where(u == 0, ahead, 1 - ahead)
        m = lax.rem(n, strips // per)
        ct_copy(loc, m // (nx - 1), lax.rem(x + 1 + lax.rem(m, nx - 1), nx), x).start()
        return 0

    for c in loads[2:6]:
        c.wait()
    chunk = slab

    def norm_part(i, acc):
        c = pl.ds(pl.multiple_of(i * chunk, chunk), chunk)
        m = W[c, :].astype(F32) + tn(A[:, c], B[...])
        return acc + fold(m * m)

    acc = lax.fori_loop(0, ny, norm_part, jnp.zeros((8, W.shape[1]), F32), unroll=4)
    NX[x] = jnp.sum(acc, axis=0, keepdims=True)
    for level in range(levels[1]):
        hear(1, level)
        if level + 1 < levels[1]:
            tell(1, level + 1)
    tell(0, 0)
    loads[1].wait()

    def to_x(name, src, slot, d):
        return copy(src, slot, leave(name), enter(name), step(1, d, nx))

    def to_y(name, src, slot, d):
        return copy(src, slot, leave(name), enter(name), step(0, d, ny))

    for d in range(1, nx):
        to_x("nx", NX.at[x], NX.at[x], d).start()
    lax.fori_loop(0, EARLY, send_ct, 0)

    SACC[...] = jnp.zeros_like(SACC)
    BG[...] = jnp.zeros_like(BG)
    R[...] = jnp.zeros_like(R)

    def low_rank():
        am = nn(A[...], W[...]) + exact(nt(A[...], A[...]), B[...].astype(F32))
        for i in range(nx):
            AM[i] = am[:, i * part : (i + 1) * part]
        AX[x] = AM[x]
        for d in range(1, nx):
            dst = lax.rem(x + d, nx)
            to_x("ax", AM.at[dst], AX.at[x], d).start()

    def project(chip):
        r = unit_rows(chip)
        t = T[r, :]
        down = nt(t, A[...]).astype(BF16)
        p = nn(t, W[...]) + nn(down, B[...])
        DB[r, :] = down
        PF[r, :] = p
        PS[r, :] = p.astype(BF16)

    def need_ct(chip):
        @pl.when(chip // per != x)
        def _():
            arrived(ct_r.at[chip], CT.at[unit_rows(chip)])

    def weighted(chip):
        r = unit_rows(chip)
        w = WT[r, :]
        return CT[r, :].astype(F32) * jnp.concatenate([w] * (W.shape[1] // 128), axis=1)

    def scale_sum(chip):
        SACC[...] += fold(weighted(chip) * PF[unit_rows(chip), :])

    def backward(chip):
        r = unit_rows(chip)
        gp = (weighted(chip) * SCALE[...]).astype(BF16)
        BG[...] += tn(DB[r, :], gp)
        back = nt(B[...], gp)
        high = back.astype(BF16)
        low = (back - high.astype(F32)).astype(BF16)
        both = nn(jnp.concatenate([high, low], axis=0), T[r, :])
        R[...] += both[: back.shape[0]] + both[back.shape[0] :]

    def to_owner(chip):
        return lax.rem(chip // per - x + nx, nx)

    passes_on = jnp.where(k == 0, 1, nx - 1)

    def slot_of(chip):
        return pl.ds(pl.multiple_of(lax.rem(chip, per) * unit, unit), unit)

    def p_out(chip):
        side = jnp.where(to_owner(chip) == 1, 0, 1)
        dst = PR.at[side, slot_of(chip)]
        return copy(PS.at[unit_rows(chip)], dst, leave("p"), enter("p"), at(1, chip // per))

    def send_p(chip):
        @pl.when((to_owner(chip) == nx - passes_on))
        def _():
            p_out(chip).start()

        @pl.when(to_owner(chip) == 2)
        def _():
            dev = at(1, lax.rem(x + passes_on, nx))
            dst = PV.at[slot_of(chip)]
            copy(PS.at[unit_rows(chip)], dst, leave("p"), pv_r.at[lax.rem(chip, per)], dev).start()

    def pass_on(chip):
        @pl.when(to_owner(chip) == passes_on)
        def _():
            slot = slot_of(chip)
            arrived(pv_r.at[lax.rem(chip, per)], PV.at[slot])
            r = unit_rows(chip)
            PS[r, :] = (PF[r, :] + PV[slot, :].astype(F32)).astype(BF16)
            p_out(chip).start()

    def handle(i):
        s = i // PIECES + 1
        h = lax.rem(i, PIECES)
        far = i >= full
        other = PIECES // 2
        hl = jnp.where(far, h + other, h)
        fr = lax.rem(z - s + nz, nz)
        fl = lax.rem(z + s, nz)
        third = i >= full - PIECES
        ring(True, fr, h, i).wait_recv()
        across(fr, h, jnp.where(far, nz - 1, 2 * s - 1)).start()

        @pl.when((i < full - PIECES) | (third & (h < other) & (i < full)))
        def _():
            ring(True, fr, h, i + PIECES).start()

        ring(False, fl, hl, i).wait_recv()
        across(fl, hl, jnp.where(far, nz - 1, 2 * s)).start()

        @pl.when((i < full - PIECES) | (third & (h >= other) & (i < full)))
        def _():
            ring(False, fl, hl, jnp.where(third, i + PIECES - other, i + PIECES)).start()

        @pl.when(i + EARLY < strips)
        def _():
            send_ct(i + EARLY, 0)

    def need_tokens(j):
        arrived(d_r.at[j], T.at[token_rows(chip_of(j), 1 - k, 0, rows)])

    def handle_range(low, high):
        def one(i, _):
            handle(i)
            return 0

        lax.fori_loop(low, high, one, 0)

    held = HELD

    def settle(j, _):
        c = chip_of(j)
        need_ct(c)
        scale_sum(c)
        backward(c)
        return 0

    def slice_weights():
        cols = pl.ds(pl.multiple_of(y * slab, slab), slab)
        wide = W.shape[1]
        low_rank_t = tn(B[...], A[:, cols])
        high = low_rank_t.astype(BF16)
        WX[:wide, :] = W[cols, :].astype(F32).T.astype(BF16)
        WX[wide : 2 * wide, :] = high
        WX[2 * wide :, :] = (low_rank_t - high.astype(F32)).astype(BF16)

    need_tokens(0)
    project(z)
    handle_range(0, PIECES // 4)
    low_rank()
    handle_range(PIECES // 4, 3 * PIECES // 4)
    slice_weights()
    handle_range(3 * PIECES // 4, PIECES)
    send_p(z)

    def turn(j, _):
        s = (j + 1) // 2
        odd = lax.rem(j, 2)
        chip = chip_of(j)

        @pl.when(odd == 1)
        def _():
            handle(s * PIECES)

        need_tokens(j)
        project(chip)

        @pl.when(j == 1)
        def _():
            arrived(enter("nx"), NX.at[pl.ds(0, nx - 1)])
            sq = NX[0]
            for i in range(1, nx):
                sq = sq + NX[i]
            norm = jnp.sqrt(sq + EPS)
            NORM[...] = norm
            SCALE[...] = MAG[...] / norm

        mid = s * PIECES + PIECES // 2
        low = jnp.minimum(jnp.where(odd == 1, s * PIECES + 1, mid), pieces)
        high = jnp.minimum(jnp.where(odd == 1, mid, mid + 1), pieces)
        handle_range(low, high)

        for level in range(max(levels.values())):

            @pl.when(j == level + 1)
            def _():
                spread_word(level)

        @pl.when(j < held)
        def _():
            send_p(chip)

        @pl.when((j >= 2) & (j < nz - 3))
        def _():
            settle(j - 2, 0)

        handle_range(high, jnp.where(odd == 1, high, jnp.minimum((s + 1) * PIECES, pieces)))

        @pl.when((j >= 2) & (j < nz - 3))
        def _():
            pass_on(chip_of(j - 2))

        @pl.when(j == nz - 4)
        def _():
            pass_on(chip_of(j - 1))
            lax.fori_loop(nz - 5, nz - 3, settle, 0)
            for i in range(ny):
                H[i] = R[:, i * slab : (i + 1) * slab]
            R[...] = jnp.zeros_like(R)
            RY[y] = H[y]
            for d in far_first(ny):
                dst = lax.rem(y + d, ny)
                to_y("ry", H.at[dst], RY.at[y], d).start()

        return 0

    lax.fori_loop(1, nz - 1, turn, 0)
    for j in (nz - 3, nz - 2):
        need_ct(chip_of(j))
        scale_sum(chip_of(j))
    need_tokens(nz - 1)
    project(chip_of(nz - 1))

    need_ct(chip_of(nz - 1))
    scale_sum(chip_of(nz - 1))
    me = y * nx + x
    SS[me] = jnp.sum(SACC[...], axis=0, keepdims=True)
    away = [(dy, dx) for dy in range(ny) for dx in range(nx) if dy or dx]
    for dy, dx in sorted(away, key=lambda o: -min(o[0], ny - o[0]) - min(o[1], nx - o[1])):
        dev = (lax.rem(y + dy, ny), lax.rem(x + dx, nx), z, k)
        copy(SS.at[me], SS.at[me], leave("s"), enter("s"), dev).start()

    def finish_b(j, _):
        backward(chip_of(j))
        return 0

    lax.fori_loop(nz - 3, nz, finish_b, 0)
    for i in range(ny):
        HL[i] = R[:, i * slab : (i + 1) * slab].astype(BF16)
    RL[y] = HL[y]
    for d in far_first(ny):
        dst = lax.rem(y + d, ny)
        to_y("rl", HL.at[dst], RL.at[y], d).start()
    for i in range(nx):
        BGS[i] = BG[:, i * part : (i + 1) * part]
    BX[x] = BGS[x]

    for d in range(1, nx):
        dst = lax.rem(x + d, nx)
        to_x("bx", BGS.at[dst], BX.at[x], d).start()

    def send_held(j, _):
        send_p(chip_of(j))
        return 0

    lax.fori_loop(held, nz, send_held, 0)
    pass_on(chip_of(held - 1))

    arrived(enter("ry"), RY.at[pl.ds(0, ny - 1)])
    row_part = RY[0]
    for i in range(1, ny):
        row_part = row_part + RY[i]
    norm = NORM[...]
    inverse = 1.0 / norm
    slope = -MAG[...] * (inverse * inverse * inverse)

    arrived(enter("s"), SS.at[pl.ds(0, nx * ny - 1)])
    s_all = SS[0]
    for i in range(1, nx * ny):
        s_all = s_all + SS[i]
    coef = s_all * slope
    scaled = (B[...].astype(F32) * coef).astype(BF16)
    part_y = nn(jnp.concatenate([scaled] * 3, axis=1), WX[...])
    arrived(enter("rl"), RL.at[pl.ds(0, ny - 1)])
    for i in range(ny):
        row_part = row_part + RL[i].astype(F32)
    part_y = part_y + row_part

    for i in range(2):
        CX[i] = part_y[:, i * lane : (i + 1) * lane].astype(BF16)
    here = 2 * z + k
    ZX[here] = CX[k]
    for d in far_first(nz) + [0]:
        for other in (0, 1):
            if d or other:
                core = k if other == 0 else 1 - k
                dev = (y, x, lax.rem(z + d, nz), core)
                copy(CX.at[core], ZX.at[here], leave("zx"), enter("zx"), dev).start()
    gmag_ref[...] = s_all * inverse

    def pass_held(j, _):
        pass_on(chip_of(j))
        return 0


    arrived(enter("bx"), BX.at[pl.ds(0, nx - 1)])
    bx = BX[0]
    for i in range(1, nx):
        bx = bx + BX[i]
    BY[y] = bx
    for d in far_first(ny):
        to_y("by", BY.at[y], BY.at[y], d).start()
    lax.fori_loop(held, nz, pass_held, 0)
    arrived(enter("ax"), AX.at[pl.ds(0, nx - 1)])
    a_all = AX[0]
    for i in range(1, nx):
        a_all = a_all + AX[i]

    arrived(enter("zx"), ZX.at[pl.ds(0, 2 * nz - 1)])
    whole = ZX[0].astype(F32)
    for i in range(1, 2 * nz):
        whole = whole + ZX[i].astype(F32)
    spot = 2 * y + k
    IF[spot] = whole.astype(BF16)
    for d in far_first(ny) + [0]:
        for other in (0, 1):
            if d or other:
                dev = (lax.rem(y + d, ny), x, z, k if other == 0 else 1 - k)
                copy(IF.at[spot], IF.at[spot], leave("if"), enter("if"), dev).start()

    arrived(enter("p"), PR)
    rest = pl.ds(pl.multiple_of(x * own, own), own)
    total = PF[rest, :]
    for side in range(2):
        total = total + PR[side].astype(F32)
    proj_ref[...] = (total * SCALE[...]).astype(BF16)

    arrived(enter("by"), BY.at[pl.ds(0, ny - 1)])
    b_all = BY[0]
    for i in range(1, ny):
        b_all = b_all + BY[i]

    for i in range(nx):

        @pl.when(x == i)
        def _():
            c = slice(i * part, (i + 1) * part)
            gb_ref[:, c] = b_all + a_all * coef[:, c]

    def gb_part(i):
        return gb_ref.at[:, pl.ds(pl.multiple_of(i * part, part), part)]

    for d in range(1, nx):
        to_x("bo", gb_part(x), gb_part(x), d).start()

    arrived(enter("bo"), gb_ref.at[:, pl.ds(0, (nx - 1) * part)])
    arrived(enter("if"), IF.at[pl.ds(0, 2 * ny - 1)])
    for i in range(2 * ny):
        ifg_ref[:, i * lane : (i + 1) * lane] = IF[i].astype(F32)

    def sent(name, ref):
        copy(ref, ref, leave(name), leave(name), partner).wait_send()

    sent("zr", T.at[pl.ds(0, pieces * piece)])
    sent("zl", T.at[pl.ds(0, pieces * piece)])
    sent("d", T.at[pl.ds(0, 2 * pieces * piece)])
    sent("own", T.at[pl.ds(0, rows)])
    sent("ct", CT.at[pl.ds(0, (nx - 1) * own)])
    sent("p", PS.at[pl.ds(0, (nx - 1) * own)])
    sent("nx", NX.at[pl.ds(0, nx - 1)])
    sent("ax", AX.at[pl.ds(0, nx - 1)])
    sent("s", SS.at[pl.ds(0, nx * ny - 1)])
    sent("bx", BX.at[pl.ds(0, nx - 1)])
    sent("by", BY.at[pl.ds(0, ny - 1)])
    sent("bo", gb_ref.at[:, pl.ds(0, (nx - 1) * part)])
    sent("ry", RY.at[pl.ds(0, ny - 1)])
    sent("rl", RL.at[pl.ds(0, ny - 1)])
    sent("zx", ZX.at[pl.ds(0, 2 * nz - 1)])
    sent("if", IF.at[pl.ds(0, 2 * ny - 1)])


def put_out(*refs):
    *pairs, sem = refs
    copies = [pltpu.make_async_copy(pairs[i], pairs[i + 4], sem.at[i]) for i in range(4)]
    for c in copies:
        c.start()
    for c in copies:
        c.wait()


def per_device(sizes, tokens, weight, a, b, magnitude, cotangent, lengths):
    ny, nx, nz = sizes
    rows, feats = tokens.shape
    rank, cols = b.shape
    group = rows * 2 * nz
    own = group // nx
    slab = feats // ny
    part = cols // nx
    per = nz // nx
    ring = (nz // 2 - 1) * PIECES + PIECES // 2
    words = ny // 2 + nx // 2 + nz // 2 - 2
    V = pltpu.VMEM
    S = lambda n: pltpu.SemaphoreType.DMA((n,))
    outs = pl.pallas_call(
        functools.partial(kernel, sizes),
        out_shape=(
            V((own, cols), BF16),
            V((1, cols), F32),
            V((rank, feats), F32),
            V((rank, cols), F32),
        ),
        in_specs=[pl.BlockSpec(memory_space=pl.ANY)] * 7,
        out_specs=[pl.BlockSpec(memory_space=pltpu.VMEM)] * 4,
        scratch_shapes=[
            V((group, feats), BF16),
            V((feats, cols), BF16),
            V((rank, feats), BF16),
            V((rank, cols), BF16),
            V((group, cols), BF16),
            V((group, 128), F32),
            V((group, cols), F32),
            V((group, cols), BF16),
            V((2, own, cols), BF16),
            V((own, cols), BF16),
            V((group, rank), BF16),
            V((nx, 1, cols), F32),
            V((nx, rank, part), F32),
            V((8, cols), F32),
            V((nx * ny, 1, cols), F32),
            V((1, cols), F32),
            V((1, cols), F32),
            V((rank, cols), F32),
            V((nx, rank, part), F32),
            V((nx, rank, part), F32),
            V((ny, rank, part), F32),
            V((rank, feats), F32),
            V((ny, rank, slab), F32),
            V((ny, rank, slab), F32),
            V((ny, rank, slab), BF16),
            V((ny, rank, slab), BF16),
            V((2, rank, slab // 2), BF16),
            V((2 * nz, rank, slab // 2), BF16),
            V((2 * ny, rank, slab // 2), BF16),
            V((nx, rank, part), F32),
            V((3 * cols, slab), BF16),
            V((1, cols), F32),
            pltpu.SMEM(lengths.shape, jnp.int32),
            S(7),
            S(ring), S(ring),
            S(nz), S(nz), S(per),
            S(len(LEAVE)), S(len(ENTER)),
            pltpu.SemaphoreType.REGULAR((words,)),
        ],
        compiler_params=pltpu.CompilerParams(
            collective_id=0, has_side_effects=True, vmem_limit_bytes=56 * 1024 * 1024
        ),
        name="lora_step",
    )(tokens, weight, a, b, magnitude.reshape(1, cols), cotangent, lengths)
    whole = [jax.ShapeDtypeStruct(o.shape, o.dtype) for o in outs]
    proj, gmag, ifg, gb = pl.pallas_call(
        put_out,
        out_shape=whole,
        in_specs=[pl.BlockSpec(memory_space=pltpu.VMEM)] * 4,
        out_specs=[pl.BlockSpec(memory_space=pl.ANY)] * 4,
        scratch_shapes=[S(4)],
        compiler_params=pltpu.CompilerParams(vmem_limit_bytes=1024 * 1024),
        name="put_out",
    )(*outs)
    return proj, gmag.reshape(cols), ifg, gb


def solution(mesh):
    ny, nx = mesh.shape["dp"], mesh.shape["row"]
    nz = mesh.shape["col"] // 2
    split = Mesh(mesh.devices.reshape(ny, nx, nz, 2), AXES)
    return jax.shard_map(
        functools.partial(per_device, (ny, nx, nz)),
        mesh=split,
        in_specs=(
            P(("dp", "z", "core"), "row"),
            P("row", COL),
            P(None, "row"),
            P(None, COL),
            P(COL),
            P(("dp", "row"), COL),
            P("dp", None),
        ),
        out_specs=(P(("dp", "row"), COL), P(COL), P(None, "row"), P(None, COL)),
        check_vma=False,
    )
```

```python
import functools

import jax
import jax.numpy as jnp
from jax import lax
from jax.experimental import pallas as pl
from jax.experimental.pallas import tpu as pltpu
from jax.sharding import Mesh
from jax.sharding import PartitionSpec as P

AXES = ("dp", "row", "z", "core")
COL = ("z", "core")
EPS = 1e-06
F32 = jnp.float32
BF16 = jnp.bfloat16
HIGHEST = lax.Precision.HIGHEST
HELD = 5
PIECES = 4
EARLY = 6


TOKEN = "own"
SAME = ("zr", "zl", "d", "own")
LEAVE = ("own", "ct", "p", "nx", "ax", "s", "bx", "by", "bo", "ry", "rl", "zx", "if")
ENTER = ("p", "nx", "ax", "s", "bx", "by", "bo", "ry", "rl", "zx", "if")


def nn(a, b):
    return lax.dot_general(a, b, (((1,), (0,)), ((), ())), preferred_element_type=F32)


def nt(a, b):
    return lax.dot_general(a, b, (((1,), (1,)), ((), ())), preferred_element_type=F32)


def tn(a, b):
    return lax.dot_general(a, b, (((0,), (0,)), ((), ())), preferred_element_type=F32)


def exact(a, b):
    return lax.dot_general(
        a, b, (((1,), (0,)), ((), ())), preferred_element_type=F32, precision=HIGHEST
    )


def far_first(n):
    return sorted(range(1, n), key=lambda d: -min(d, n - d))


def fold(a):
    return jnp.sum(a.reshape(a.shape[0] // 8, 8, a.shape[1]), axis=0)


def kernel(
    sizes,
    tok_hbm, w_hbm, a_hbm, b_hbm, mag_hbm, ct_hbm, lens_hbm,
    proj_ref, gmag_ref, ifg_ref, gb_ref,
    T, W, A, B, CT, WT, PF, PS, PR, PV, DB,
    NX, AX, SACC, SS, SCALE, NORM, BG, BGS, BX, BY, R, RY, H, RL, HL, CX, ZX, IF, AM, WX, MAG, LENS,
    load_sem, zr_r, zl_r, d_r, ct_r, pv_r, out_sem, in_sem, wave,
):
    ny, nx, nz = sizes
    y, x, z, k = (lax.axis_index(a) for a in AXES)
    rows = tok_hbm.shape[0]
    piece = rows // PIECES
    unit = 2 * rows
    own = nz // nx * unit
    per = nz // nx
    slab = T.shape[1] // ny
    lane = slab // 2
    part = W.shape[1] // nx

    def at(axis, index):
        return tuple(index if i == axis else v for i, v in enumerate((y, x, z, k)))

    def step(axis, by, n):
        return at(axis, lax.rem((y, x, z)[axis] + by + n, n))

    def leave(name):
        return out_sem.at[LEAVE.index(TOKEN if name in SAME else name)]

    def enter(name):
        return in_sem.at[ENTER.index(name)]

    partner = (y, x, z, 1 - k)
    right = step(2, 1, nz)
    left = step(2, -1, nz)

    def copy(src, dst, ssem, rsem, dev):
        return pltpu.make_async_remote_copy(
            src_ref=src, dst_ref=dst, send_sem=ssem, recv_sem=rsem,
            device_id=dev, device_id_type=pl.DeviceIdType.MESH,
        )

    def arrived(sem, ref):
        copy(ref, ref, sem, sem, partner).wait_recv()

    def token_rows(chip, core, h, n):
        return pl.ds(pl.multiple_of(chip * unit + core * rows + h * piece, piece), n)

    mine = token_rows(z, k, 0, rows)
    owned = pl.ds(pl.multiple_of(x * own, own), own)
    loads = [
        pltpu.make_async_copy(ct_hbm, CT.at[owned], load_sem.at[0]),
        pltpu.make_async_copy(a_hbm, A, load_sem.at[1]),
        pltpu.make_async_copy(b_hbm, B, load_sem.at[2]),
        pltpu.make_async_copy(w_hbm, W, load_sem.at[3]),
        pltpu.make_async_copy(mag_hbm, MAG, load_sem.at[4]),
        pltpu.make_async_copy(lens_hbm, LENS, load_sem.at[5]),
    ]
    first = [
        pltpu.make_async_copy(
            tok_hbm.at[pl.ds(h * piece, piece)], T.at[token_rows(z, k, h, piece)], load_sem.at[6 + h]
        )
        for h in range(PIECES)
    ]
    for c in first + loads:
        c.start()

    barrier = pltpu.get_barrier_semaphore()
    near = [partner] + [step(axis, d, n) for axis, n in ((2, nz), (1, nx), (0, ny)) for d in (1, -1)]

    def signal(sem, dev):
        pl.semaphore_signal(sem, inc=1, device_id=dev, device_id_type=pl.DeviceIdType.MESH)

    for dev in near:
        signal(barrier, dev)

    seqs = LENS.shape[1]

    def weigh(i, _):
        pos = lax.broadcasted_iota(jnp.int32, (unit, 128), 0) + i * unit
        total = jnp.zeros((unit, 128), F32)
        start = jnp.int32(0)
        for s in range(seqs):
            length = LENS[0, s]
            end = start + length
            inverse = 1.0 / jnp.full((1, 128), length, jnp.int32).astype(F32)
            total += jnp.where((pos >= start) & (pos < end), inverse, 0.0)
            start = end
        WT[pl.ds(pl.multiple_of(i * unit, unit), unit), :] = total
        return 0

    pl.semaphore_wait(barrier, len(near))

    def ring(right_way, src_chip, h, idx):
        r = token_rows(src_chip, k, h, piece)
        if right_way:
            return copy(T.at[r], T.at[r], leave("zr"), zr_r.at[idx], right)
        return copy(T.at[r], T.at[r], leave("zl"), zl_r.at[idx], left)

    def across(src_chip, h, j):
        r = token_rows(src_chip, k, h, piece)
        return copy(T.at[r], T.at[r], leave("d"), d_r.at[j], partner)

    full = (nz // 2 - 1) * PIECES
    pieces = full + PIECES // 2
    for h in range(PIECES):
        first[h].wait()
        ring(True, z, h, h).start()
        ring(False, z, h, h).start()
    copy(T.at[mine], T.at[mine], leave("own"), d_r.at[0], partner).start()

    levels = {0: ny // 2, 1: nx // 2 - 1, 2: nz // 2 - 1}
    base = {1: 0, 0: levels[1], 2: levels[1] + levels[0]}

    def tell(axis, level):
        for d in (1, -1):
            signal(wave.at[base[axis] + level], step(axis, d, (ny, nx, nz)[axis]))

    def hear(axis, level):
        pl.semaphore_wait(wave.at[base[axis] + level], 2)

    tell(1, 0)
    tell(2, 0)
    loads[5].wait()
    lax.fori_loop(0, nz, weigh, 0)
    def spread_word(level):
        for axis in (0, 2):
            if level < levels[axis]:
                hear(axis, level)
            if level + 1 < levels[axis]:
                tell(axis, level + 1)

    def chip_of(j):
        s = (j + 1) // 2
        return lax.rem(z + nz + jnp.where(lax.rem(j, 2) == 1, -s, s), nz)

    def unit_rows(chip):
        return pl.ds(pl.multiple_of(chip * unit, unit), unit)

    def turn_of(chip):
        d = lax.rem(chip - z + nz, nz)
        return jnp.where(d < nz // 2, 2 * d, 2 * (nz - d) - 1)

    ahead = jnp.where(turn_of(x * per) < turn_of(x * per + 1), 0, 1)
    strip = unit // 2
    strips = per * 2 * (nx - 1)

    def ct_copy(loc, part_of, dx, src_x):
        r = pl.ds(pl.multiple_of((src_x * per + loc) * unit + part_of * strip, strip), strip)
        d = lax.rem(dx - src_x + nx, nx)
        return copy(CT.at[r], CT.at[r], leave("ct"), ct_r.at[src_x * per + loc], at(1, dx))

    def send_ct(n, _):
        u = n // (strips // per)
        loc = jnp.where(u == 0, ahead, 1 - ahead)
        m = lax.rem(n, strips // per)
        ct_copy(loc, m // (nx - 1), lax.rem(x + 1 + lax.rem(m, nx - 1), nx), x).start()
        return 0

    for c in loads[1:5]:
        c.wait()
    chunk = slab

    def norm_part(i, acc):
        c = pl.ds(pl.multiple_of(i * chunk, chunk), chunk)
        m = W[c, :].astype(F32) + tn(A[:, c], B[...])
        return acc + fold(m * m)

    acc = lax.fori_loop(0, ny, norm_part, jnp.zeros((8, W.shape[1]), F32), unroll=4)
    NX[x] = jnp.sum(acc, axis=0, keepdims=True)
    for level in range(levels[1]):
        hear(1, level)
        if level + 1 < levels[1]:
            tell(1, level + 1)
    tell(0, 0)
    loads[0].wait()

    def to_x(name, src, slot, d):
        return copy(src, slot, leave(name), enter(name), step(1, d, nx))

    def to_y(name, src, slot, d):
        return copy(src, slot, leave(name), enter(name), step(0, d, ny))

    for d in range(1, nx):
        to_x("nx", NX.at[x], NX.at[x], d).start()
    lax.fori_loop(0, EARLY, send_ct, 0)

    SACC[...] = jnp.zeros_like(SACC)
    BG[...] = jnp.zeros_like(BG)
    R[...] = jnp.zeros_like(R)

    def low_rank():
        am = nn(A[...], W[...]) + exact(nt(A[...], A[...]), B[...].astype(F32))
        for i in range(nx):
            AM[i] = am[:, i * part : (i + 1) * part]
        AX[x] = AM[x]
        for d in range(1, nx):
            dst = lax.rem(x + d, nx)
            to_x("ax", AM.at[dst], AX.at[x], d).start()

    def project(chip):
        r = unit_rows(chip)
        t = T[r, :]
        down = nt(t, A[...]).astype(BF16)
        p = nn(t, W[...]) + nn(down, B[...])
        DB[r, :] = down
        PF[r, :] = p
        PS[r, :] = p.astype(BF16)

    def need_ct(chip):
        @pl.when(chip // per != x)
        def _():
            arrived(ct_r.at[chip], CT.at[unit_rows(chip)])

    def weighted(chip):
        r = unit_rows(chip)
        w = WT[r, :]
        return CT[r, :].astype(F32) * jnp.concatenate([w] * (W.shape[1] // 128), axis=1)

    def scale_sum(chip):
        SACC[...] += fold(weighted(chip) * PF[unit_rows(chip), :])

    def backward(chip):
        r = unit_rows(chip)
        gp = (weighted(chip) * SCALE[...]).astype(BF16)
        BG[...] += tn(DB[r, :], gp)
        back = nt(B[...], gp)
        high = back.astype(BF16)
        low = (back - high.astype(F32)).astype(BF16)
        both = nn(jnp.concatenate([high, low], axis=0), T[r, :])
        R[...] += both[: back.shape[0]] + both[back.shape[0] :]

    def to_owner(chip):
        return lax.rem(chip // per - x + nx, nx)

    passes_on = jnp.where(k == 0, 1, nx - 1)

    def slot_of(chip):
        return pl.ds(pl.multiple_of(lax.rem(chip, per) * unit, unit), unit)

    def p_out(chip):
        side = jnp.where(to_owner(chip) == 1, 0, 1)
        dst = PR.at[side, slot_of(chip)]
        return copy(PS.at[unit_rows(chip)], dst, leave("p"), enter("p"), at(1, chip // per))

    def send_p(chip):
        @pl.when((to_owner(chip) == nx - passes_on))
        def _():
            p_out(chip).start()

        @pl.when(to_owner(chip) == 2)
        def _():
            dev = at(1, lax.rem(x + passes_on, nx))
            dst = PV.at[slot_of(chip)]
            copy(PS.at[unit_rows(chip)], dst, leave("p"), pv_r.at[lax.rem(chip, per)], dev).start()

    def pass_on(chip):
        @pl.when(to_owner(chip) == passes_on)
        def _():
            slot = slot_of(chip)
            arrived(pv_r.at[lax.rem(chip, per)], PV.at[slot])
            r = unit_rows(chip)
            PS[r, :] = (PF[r, :] + PV[slot, :].astype(F32)).astype(BF16)
            p_out(chip).start()

    def handle(i):
        s = i // PIECES + 1
        h = lax.rem(i, PIECES)
        far = i >= full
        other = PIECES // 2
        hl = jnp.where(far, h + other, h)
        fr = lax.rem(z - s + nz, nz)
        fl = lax.rem(z + s, nz)
        third = i >= full - PIECES
        ring(True, fr, h, i).wait_recv()
        across(fr, h, jnp.where(far, nz - 1, 2 * s - 1)).start()

        @pl.when((i < full - PIECES) | (third & (h < other) & (i < full)))
        def _():
            ring(True, fr, h, i + PIECES).start()

        ring(False, fl, hl, i).wait_recv()
        across(fl, hl, jnp.where(far, nz - 1, 2 * s)).start()

        @pl.when((i < full - PIECES) | (third & (h >= other) & (i < full)))
        def _():
            ring(False, fl, hl, jnp.where(third, i + PIECES - other, i + PIECES)).start()

        @pl.when(i + EARLY < strips)
        def _():
            send_ct(i + EARLY, 0)

    def need_tokens(j):
        arrived(d_r.at[j], T.at[token_rows(chip_of(j), 1 - k, 0, rows)])

    def handle_range(low, high):
        def one(i, _):
            handle(i)
            return 0

        lax.fori_loop(low, high, one, 0)

    held = HELD

    def settle(j, _):
        c = chip_of(j)
        need_ct(c)
        scale_sum(c)
        backward(c)
        return 0

    def slice_weights():
        cols = pl.ds(pl.multiple_of(y * slab, slab), slab)
        wide = W.shape[1]
        low_rank_t = tn(B[...], A[:, cols])
        high = low_rank_t.astype(BF16)
        WX[:wide, :] = W[cols, :].astype(F32).T.astype(BF16)
        WX[wide : 2 * wide, :] = high
        WX[2 * wide :, :] = (low_rank_t - high.astype(F32)).astype(BF16)

    need_tokens(0)
    project(z)
    handle_range(0, PIECES // 4)
    low_rank()
    handle_range(PIECES // 4, 3 * PIECES // 4)
    slice_weights()
    handle_range(3 * PIECES // 4, PIECES)
    send_p(z)

    def turn(j, _):
        s = (j + 1) // 2
        odd = lax.rem(j, 2)
        chip = chip_of(j)

        @pl.when((odd == 1) & (j < nz - 3))
        def _():
            handle(s * PIECES)

        need_tokens(j)
        project(chip)

        @pl.when(j == 1)
        def _():
            arrived(enter("nx"), NX.at[pl.ds(0, nx - 1)])
            sq = NX[0]
            for i in range(1, nx):
                sq = sq + NX[i]
            norm = jnp.sqrt(sq + EPS)
            NORM[...] = norm
            SCALE[...] = MAG[...] / norm

        mid = s * PIECES + PIECES // 2
        low = jnp.minimum(jnp.where(odd == 1, s * PIECES + 1, mid), full)
        high = jnp.minimum(jnp.where(odd == 1, mid, mid + 1), full)
        low = jnp.where(j == nz - 3, full, low)
        high = jnp.where(j == nz - 3, pieces, high)
        handle_range(low, high)

        for level in range(max(levels.values())):

            @pl.when(j == level + 1)
            def _():
                spread_word(level)

        @pl.when(j < held)
        def _():
            send_p(chip)

        @pl.when((j >= 2) & (j < nz - 3))
        def _():
            settle(j - 2, 0)

        handle_range(high, jnp.where(odd == 1, high, jnp.minimum((s + 1) * PIECES, full)))

        @pl.when((j >= 2) & (j < nz - 3))
        def _():
            pass_on(chip_of(j - 2))

        @pl.when(j == nz - 4)
        def _():
            lax.fori_loop(nz - 5, nz - 3, settle, 0)
            for i in range(ny):
                H[i] = R[:, i * slab : (i + 1) * slab]
            R[...] = jnp.zeros_like(R)
            RY[y] = H[y]
            for d in far_first(ny):
                dst = lax.rem(y + d, ny)
                to_y("ry", H.at[dst], RY.at[y], d).start()

        return 0

    lax.fori_loop(1, nz - 1, turn, 0)
    for j in (nz - 3, nz - 2):
        need_ct(chip_of(j))
        scale_sum(chip_of(j))
    need_tokens(nz - 1)
    project(chip_of(nz - 1))

    need_ct(chip_of(nz - 1))
    scale_sum(chip_of(nz - 1))
    me = y * nx + x
    SS[me] = jnp.sum(SACC[...], axis=0, keepdims=True)
    away = [(dy, dx) for dy in range(ny) for dx in range(nx) if dy or dx]
    for dy, dx in sorted(away, key=lambda o: -min(o[0], ny - o[0]) - min(o[1], nx - o[1])):
        dev = (lax.rem(y + dy, ny), lax.rem(x + dx, nx), z, k)
        copy(SS.at[me], SS.at[me], leave("s"), enter("s"), dev).start()

    def finish_b(j, _):
        backward(chip_of(j))
        return 0

    lax.fori_loop(nz - 3, nz, finish_b, 0)
    for i in range(ny):
        HL[i] = R[:, i * slab : (i + 1) * slab].astype(BF16)
    RL[y] = HL[y]
    for d in far_first(ny):
        dst = lax.rem(y + d, ny)
        to_y("rl", HL.at[dst], RL.at[y], d).start()
    for i in range(nx):
        BGS[i] = BG[:, i * part : (i + 1) * part]
    BX[x] = BGS[x]

    for d in range(1, nx):
        dst = lax.rem(x + d, nx)
        to_x("bx", BGS.at[dst], BX.at[x], d).start()

    def send_held(j, _):
        send_p(chip_of(j))
        return 0

    lax.fori_loop(held, nz, send_held, 0)
    for j in (held - 2, held - 1):
        pass_on(chip_of(j))

    arrived(enter("ry"), RY.at[pl.ds(0, ny - 1)])
    row_part = RY[0]
    for i in range(1, ny):
        row_part = row_part + RY[i]
    norm = NORM[...]
    inverse = 1.0 / norm
    slope = -MAG[...] * (inverse * inverse * inverse)

    arrived(enter("s"), SS.at[pl.ds(0, nx * ny - 1)])
    s_all = SS[0]
    for i in range(1, nx * ny):
        s_all = s_all + SS[i]
    coef = s_all * slope
    scaled = (B[...].astype(F32) * coef).astype(BF16)
    part_y = nn(jnp.concatenate([scaled] * 3, axis=1), WX[...])
    arrived(enter("rl"), RL.at[pl.ds(0, ny - 1)])
    for i in range(ny):
        row_part = row_part + RL[i].astype(F32)
    part_y = part_y + row_part

    for i in range(2):
        CX[i] = part_y[:, i * lane : (i + 1) * lane].astype(BF16)
    here = 2 * z + k
    ZX[here] = CX[k]
    for d in far_first(nz) + [0]:
        for other in (0, 1):
            if d or other:
                core = k if other == 0 else 1 - k
                dev = (y, x, lax.rem(z + d, nz), core)
                copy(CX.at[core], ZX.at[here], leave("zx"), enter("zx"), dev).start()
    gmag_ref[...] = s_all * inverse

    def pass_held(j, _):
        pass_on(chip_of(j))
        return 0


    arrived(enter("bx"), BX.at[pl.ds(0, nx - 1)])
    bx = BX[0]
    for i in range(1, nx):
        bx = bx + BX[i]
    BY[y] = bx
    for d in far_first(ny):
        to_y("by", BY.at[y], BY.at[y], d).start()
    lax.fori_loop(held, nz, pass_held, 0)
    arrived(enter("ax"), AX.at[pl.ds(0, nx - 1)])
    a_all = AX[0]
    for i in range(1, nx):
        a_all = a_all + AX[i]

    arrived(enter("zx"), ZX.at[pl.ds(0, 2 * nz - 1)])
    whole = ZX[0].astype(F32)
    for i in range(1, 2 * nz):
        whole = whole + ZX[i].astype(F32)
    spot = 2 * y + k
    IF[spot] = whole.astype(BF16)
    for d in far_first(ny) + [0]:
        for other in (0, 1):
            if d or other:
                dev = (lax.rem(y + d, ny), x, z, k if other == 0 else 1 - k)
                copy(IF.at[spot], IF.at[spot], leave("if"), enter("if"), dev).start()

    arrived(enter("p"), PR)
    rest = pl.ds(pl.multiple_of(x * own, own), own)
    total = PF[rest, :]
    for side in range(2):
        total = total + PR[side].astype(F32)
    proj_ref[...] = (total * SCALE[...]).astype(BF16)

    arrived(enter("by"), BY.at[pl.ds(0, ny - 1)])
    b_all = BY[0]
    for i in range(1, ny):
        b_all = b_all + BY[i]

    for i in range(nx):

        @pl.when(x == i)
        def _():
            c = slice(i * part, (i + 1) * part)
            gb_ref[:, c] = b_all + a_all * coef[:, c]

    def gb_part(i):
        return gb_ref.at[:, pl.ds(pl.multiple_of(i * part, part), part)]

    for d in range(1, nx):
        to_x("bo", gb_part(x), gb_part(x), d).start()

    arrived(enter("bo"), gb_ref.at[:, pl.ds(0, (nx - 1) * part)])
    arrived(enter("if"), IF.at[pl.ds(0, 2 * ny - 1)])
    for i in range(2 * ny):
        ifg_ref[:, i * lane : (i + 1) * lane] = IF[i].astype(F32)

    def sent(name, ref):
        copy(ref, ref, leave(name), leave(name), partner).wait_send()

    sent("own", T.at[pl.ds(0, 4 * pieces * piece + rows)])
    sent("ct", CT.at[pl.ds(0, (nx - 1) * own)])
    sent("p", PS.at[pl.ds(0, (nx - 1) * own)])
    sent("nx", NX.at[pl.ds(0, nx - 1)])
    sent("ax", AX.at[pl.ds(0, nx - 1)])
    sent("s", SS.at[pl.ds(0, nx * ny - 1)])
    sent("bx", BX.at[pl.ds(0, nx - 1)])
    sent("by", BY.at[pl.ds(0, ny - 1)])
    sent("bo", gb_ref.at[:, pl.ds(0, (nx - 1) * part)])
    sent("ry", RY.at[pl.ds(0, ny - 1)])
    sent("rl", RL.at[pl.ds(0, ny - 1)])
    sent("zx", ZX.at[pl.ds(0, 2 * nz - 1)])
    sent("if", IF.at[pl.ds(0, 2 * ny - 1)])


def put_out(*refs):
    *pairs, sem = refs
    copies = [pltpu.make_async_copy(pairs[i], pairs[i + 4], sem.at[i]) for i in range(4)]
    for c in copies:
        c.start()
    for c in copies:
        c.wait()


def per_device(sizes, tokens, weight, a, b, magnitude, cotangent, lengths):
    ny, nx, nz = sizes
    rows, feats = tokens.shape
    rank, cols = b.shape
    group = rows * 2 * nz
    own = group // nx
    slab = feats // ny
    part = cols // nx
    per = nz // nx
    ring = (nz // 2 - 1) * PIECES + PIECES // 2
    words = ny // 2 + nx // 2 + nz // 2 - 2
    V = pltpu.VMEM
    S = lambda n: pltpu.SemaphoreType.DMA((n,))
    outs = pl.pallas_call(
        functools.partial(kernel, sizes),
        out_shape=(
            V((own, cols), BF16),
            V((1, cols), F32),
            V((rank, feats), F32),
            V((rank, cols), F32),
        ),
        in_specs=[pl.BlockSpec(memory_space=pl.ANY)] * 7,
        out_specs=[pl.BlockSpec(memory_space=pltpu.VMEM)] * 4,
        scratch_shapes=[
            V((group, feats), BF16),
            V((feats, cols), BF16),
            V((rank, feats), BF16),
            V((rank, cols), BF16),
            V((group, cols), BF16),
            V((group, 128), F32),
            V((group, cols), F32),
            V((group, cols), BF16),
            V((2, own, cols), BF16),
            V((own, cols), BF16),
            V((group, rank), BF16),
            V((nx, 1, cols), F32),
            V((nx, rank, part), F32),
            V((8, cols), F32),
            V((nx * ny, 1, cols), F32),
            V((1, cols), F32),
            V((1, cols), F32),
            V((rank, cols), F32),
            V((nx, rank, part), F32),
            V((nx, rank, part), F32),
            V((ny, rank, part), F32),
            V((rank, feats), F32),
            V((ny, rank, slab), F32),
            V((ny, rank, slab), F32),
            V((ny, rank, slab), BF16),
            V((ny, rank, slab), BF16),
            V((2, rank, slab // 2), BF16),
            V((2 * nz, rank, slab // 2), BF16),
            V((2 * ny, rank, slab // 2), BF16),
            V((nx, rank, part), F32),
            V((3 * cols, slab), BF16),
            V((1, cols), F32),
            pltpu.SMEM(lengths.shape, jnp.int32),
            S(6 + PIECES),
            S(ring), S(ring),
            S(nz), S(nz), S(per),
            S(len(LEAVE)), S(len(ENTER)),
            pltpu.SemaphoreType.REGULAR((words,)),
        ],
        compiler_params=pltpu.CompilerParams(
            collective_id=0, has_side_effects=True, vmem_limit_bytes=56 * 1024 * 1024
        ),
        name="lora_step",
    )(tokens, weight, a, b, magnitude.reshape(1, cols), cotangent, lengths)
    whole = [jax.ShapeDtypeStruct(o.shape, o.dtype) for o in outs]
    proj, gmag, ifg, gb = pl.pallas_call(
        put_out,
        out_shape=whole,
        in_specs=[pl.BlockSpec(memory_space=pltpu.VMEM)] * 4,
        out_specs=[pl.BlockSpec(memory_space=pl.ANY)] * 4,
        scratch_shapes=[S(4)],
        compiler_params=pltpu.CompilerParams(vmem_limit_bytes=1024 * 1024),
        name="put_out",
    )(*outs)
    return proj, gmag.reshape(cols), ifg, gb


def solution(mesh):
    ny, nx = mesh.shape["dp"], mesh.shape["row"]
    nz = mesh.shape["col"] // 2
    split = Mesh(mesh.devices.reshape(ny, nx, nz, 2), AXES)
    return jax.shard_map(
        functools.partial(per_device, (ny, nx, nz)),
        mesh=split,
        in_specs=(
            P(("dp", "z", "core"), "row"),
            P("row", COL),
            P(None, "row"),
            P(None, COL),
            P(COL),
            P(("dp", "row"), COL),
            P("dp", None),
        ),
        out_specs=(P(("dp", "row"), COL), P(COL), P(None, "row"), P(None, COL)),
        check_vma=False,
    )
```

```python
import functools

import jax
import jax.numpy as jnp
from jax import lax
from jax.experimental import pallas as pl
from jax.experimental.pallas import tpu as pltpu
from jax.sharding import Mesh
from jax.sharding import PartitionSpec as P

AXES = ("dp", "row", "z", "core")
COL = ("z", "core")
EPS = 1e-06
F32 = jnp.float32
BF16 = jnp.bfloat16
HIGHEST = lax.Precision.HIGHEST
HELD = 5
PIECES = 4
EARLY = 6


TOKEN = "own"
SAME = ("zr", "zl", "d", "own")
LEAVE = ("own", "ct", "p", "nx", "ax", "s", "bx", "by", "bo", "ry", "rl", "zx", "if")
ENTER = ("p", "nx", "ax", "s", "bx", "by", "bo", "ry", "rl", "zx", "if")


def nn(a, b):
    return lax.dot_general(a, b, (((1,), (0,)), ((), ())), preferred_element_type=F32)


def nt(a, b):
    return lax.dot_general(a, b, (((1,), (1,)), ((), ())), preferred_element_type=F32)


def tn(a, b):
    return lax.dot_general(a, b, (((0,), (0,)), ((), ())), preferred_element_type=F32)


def exact(a, b):
    return lax.dot_general(
        a, b, (((1,), (0,)), ((), ())), preferred_element_type=F32, precision=HIGHEST
    )


def far_first(n):
    return sorted(range(1, n), key=lambda d: -min(d, n - d))


def fold(a):
    return jnp.sum(a.reshape(a.shape[0] // 8, 8, a.shape[1]), axis=0)


def kernel(
    sizes,
    tok_hbm, w_hbm, a_hbm, b_hbm, mag_hbm, ct_hbm, lens_hbm,
    proj_ref, gmag_ref, ifg_ref, gb_ref,
    T, W, A, B, CT, WT, PF, PS, PR, PV, DB,
    NX, AX, SACC, SS, SCALE, NORM, BG, BGS, BX, BY, R, RY, H, RL, HL, CX, ZX, IF, AM, WX, AT, MAG, LENS,
    load_sem, zr_r, zl_r, d_r, ct_r, pv_r, out_sem, in_sem, wave,
):
    ny, nx, nz = sizes
    y, x, z, k = (lax.axis_index(a) for a in AXES)
    rows = tok_hbm.shape[0]
    piece = rows // PIECES
    unit = 2 * rows
    own = nz // nx * unit
    per = nz // nx
    slab = T.shape[1] // ny
    lane = slab // 2
    part = W.shape[1] // nx

    def at(axis, index):
        return tuple(index if i == axis else v for i, v in enumerate((y, x, z, k)))

    def step(axis, by, n):
        return at(axis, lax.rem((y, x, z)[axis] + by + n, n))

    def leave(name):
        return out_sem.at[LEAVE.index(TOKEN if name in SAME else name)]

    def enter(name):
        return in_sem.at[ENTER.index(name)]

    partner = (y, x, z, 1 - k)
    right = step(2, 1, nz)
    left = step(2, -1, nz)

    def copy(src, dst, ssem, rsem, dev):
        return pltpu.make_async_remote_copy(
            src_ref=src, dst_ref=dst, send_sem=ssem, recv_sem=rsem,
            device_id=dev, device_id_type=pl.DeviceIdType.MESH,
        )

    def arrived(sem, ref):
        copy(ref, ref, sem, sem, partner).wait_recv()

    def token_rows(chip, core, h, n):
        return pl.ds(pl.multiple_of(chip * unit + core * rows + h * piece, piece), n)

    mine = token_rows(z, k, 0, rows)
    owned = pl.ds(pl.multiple_of(x * own, own), own)
    loads = [
        pltpu.make_async_copy(ct_hbm, CT.at[owned], load_sem.at[0]),
        pltpu.make_async_copy(a_hbm, A, load_sem.at[1]),
        pltpu.make_async_copy(b_hbm, B, load_sem.at[2]),
        pltpu.make_async_copy(w_hbm, W, load_sem.at[3]),
        pltpu.make_async_copy(mag_hbm, MAG, load_sem.at[4]),
        pltpu.make_async_copy(lens_hbm, LENS, load_sem.at[5]),
    ]
    first = [
        pltpu.make_async_copy(
            tok_hbm.at[pl.ds(h * piece, piece)], T.at[token_rows(z, k, h, piece)], load_sem.at[6 + h]
        )
        for h in range(PIECES)
    ]
    for c in first + loads:
        c.start()

    barrier = pltpu.get_barrier_semaphore()
    near = [partner] + [step(axis, d, n) for axis, n in ((2, nz), (1, nx), (0, ny)) for d in (1, -1)]

    def signal(sem, dev):
        pl.semaphore_signal(sem, inc=1, device_id=dev, device_id_type=pl.DeviceIdType.MESH)

    for dev in near:
        signal(barrier, dev)

    seqs = LENS.shape[1]

    def weigh(i, _):
        pos = lax.broadcasted_iota(jnp.int32, (unit, 128), 0) + i * unit
        total = jnp.zeros((unit, 128), F32)
        start = jnp.int32(0)
        for s in range(seqs):
            length = LENS[0, s]
            end = start + length
            inverse = 1.0 / jnp.full((1, 128), length, jnp.int32).astype(F32)
            total += jnp.where((pos >= start) & (pos < end), inverse, 0.0)
            start = end
        WT[pl.ds(pl.multiple_of(i * unit, unit), unit), :] = total
        return 0

    pl.semaphore_wait(barrier, len(near))

    def ring(right_way, src_chip, h, idx):
        r = token_rows(src_chip, k, h, piece)
        if right_way:
            return copy(T.at[r], T.at[r], leave("zr"), zr_r.at[idx], right)
        return copy(T.at[r], T.at[r], leave("zl"), zl_r.at[idx], left)

    def across(src_chip, h, j):
        r = token_rows(src_chip, k, h, piece)
        return copy(T.at[r], T.at[r], leave("d"), d_r.at[j], partner)

    full = (nz // 2 - 1) * PIECES
    pieces = full + PIECES // 2
    for h in range(PIECES):
        first[h].wait()
        if h < PIECES // 2:
            ring(True, z, h, h).start()
            ring(False, z, h, h).start()

    def rest_of_own():
        for h in range(PIECES // 2, PIECES):
            ring(True, z, h, h).start()
            ring(False, z, h, h).start()

    @pl.when(k == 0)
    def _():
        rest_of_own()

    copy(T.at[mine], T.at[mine], leave("own"), d_r.at[0], partner).start()

    levels = {0: ny // 2, 1: nx // 2 - 1, 2: nz // 2 - 1}
    base = {1: 0, 0: levels[1], 2: levels[1] + levels[0]}

    def tell(axis, level):
        for d in (1, -1):
            signal(wave.at[base[axis] + level], step(axis, d, (ny, nx, nz)[axis]))

    def hear(axis, level):
        pl.semaphore_wait(wave.at[base[axis] + level], 2)

    tell(1, 0)
    tell(2, 0)
    loads[5].wait()
    lax.fori_loop(0, nz, weigh, 0)

    @pl.when(k == 1)
    def _():
        rest_of_own()

    def spread_word(level):
        for axis in (0, 2):
            if level < levels[axis]:
                hear(axis, level)
            if level + 1 < levels[axis]:
                tell(axis, level + 1)

    def chip_of(j):
        s = (j + 1) // 2
        return lax.rem(z + nz + jnp.where(lax.rem(j, 2) == 1, -s, s), nz)

    def unit_rows(chip):
        return pl.ds(pl.multiple_of(chip * unit, unit), unit)

    def turn_of(chip):
        d = lax.rem(chip - z + nz, nz)
        return jnp.where(d < nz // 2, 2 * d, 2 * (nz - d) - 1)

    ahead = jnp.where(turn_of(x * per) < turn_of(x * per + 1), 0, 1)
    strip = unit // 2
    strips = per * 2 * (nx - 1)

    def ct_copy(loc, part_of, dx, src_x):
        r = pl.ds(pl.multiple_of((src_x * per + loc) * unit + part_of * strip, strip), strip)
        d = lax.rem(dx - src_x + nx, nx)
        return copy(CT.at[r], CT.at[r], leave("ct"), ct_r.at[src_x * per + loc], at(1, dx))

    def send_ct(n, _):
        u = n // (strips // per)
        loc = jnp.where(u == 0, ahead, 1 - ahead)
        m = lax.rem(n, strips // per)
        ct_copy(loc, m // (nx - 1), lax.rem(x + 1 + lax.rem(m, nx - 1), nx), x).start()
        return 0

    for c in loads[1:5]:
        c.wait()
    chunk = slab

    def norm_part(i, acc):
        c = pl.ds(pl.multiple_of(i * chunk, chunk), chunk)
        m = W[c, :].astype(F32) + tn(A[:, c], B[...])
        return acc + fold(m * m)

    acc = lax.fori_loop(0, ny, norm_part, jnp.zeros((8, W.shape[1]), F32), unroll=4)
    NX[x] = jnp.sum(acc, axis=0, keepdims=True)
    for level in range(levels[1]):
        hear(1, level)
        if level + 1 < levels[1]:
            tell(1, level + 1)
    tell(0, 0)
    loads[0].wait()

    def to_x(name, src, slot, d):
        return copy(src, slot, leave(name), enter(name), step(1, d, nx))

    def to_y(name, src, slot, d):
        return copy(src, slot, leave(name), enter(name), step(0, d, ny))

    for d in range(1, nx):
        to_x("nx", NX.at[x], NX.at[x], d).start()
    lax.fori_loop(0, EARLY, send_ct, 0)

    wide_a = jnp.concatenate([A[...].astype(F32), jnp.zeros((128 - A.shape[0], A.shape[1]), F32)], axis=0)
    AT[...] = wide_a.T.astype(BF16)
    SACC[...] = jnp.zeros_like(SACC)
    BG[...] = jnp.zeros_like(BG)
    R[...] = jnp.zeros_like(R)

    def low_rank():
        am = nn(A[...], W[...]) + exact(nt(A[...], A[...]), B[...].astype(F32))
        for i in range(nx):
            AM[i] = am[:, i * part : (i + 1) * part]
        AX[x] = AM[x]
        for d in range(1, nx):
            dst = lax.rem(x + d, nx)
            to_x("ax", AM.at[dst], AX.at[x], d).start()

    def project(chip):
        r = unit_rows(chip)
        t = T[r, :]
        down = nn(t, AT[...])[:, : A.shape[0]].astype(BF16)
        p = nn(t, W[...]) + nn(down, B[...])
        DB[r, :] = down
        PF[r, :] = p
        PS[r, :] = p.astype(BF16)

    def need_ct(chip):
        @pl.when(chip // per != x)
        def _():
            arrived(ct_r.at[chip], CT.at[unit_rows(chip)])

    def weighted(chip):
        r = unit_rows(chip)
        w = WT[r, :]
        return CT[r, :].astype(F32) * jnp.concatenate([w] * (W.shape[1] // 128), axis=1)

    def scale_sum(chip):
        SACC[...] += fold(weighted(chip) * PF[unit_rows(chip), :])

    def backward(chip):
        r = unit_rows(chip)
        gp = (weighted(chip) * SCALE[...]).astype(BF16)
        BG[...] += tn(DB[r, :], gp)
        back = nt(B[...], gp)
        high = back.astype(BF16)
        low = (back - high.astype(F32)).astype(BF16)
        both = nn(jnp.concatenate([high, low], axis=0), T[r, :])
        R[...] += both[: back.shape[0]] + both[back.shape[0] :]

    def to_owner(chip):
        return lax.rem(chip // per - x + nx, nx)

    passes_on = jnp.where(k == 0, 1, nx - 1)

    def slot_of(chip):
        return pl.ds(pl.multiple_of(lax.rem(chip, per) * unit, unit), unit)

    def p_out(chip):
        side = jnp.where(to_owner(chip) == 1, 0, 1)
        dst = PR.at[side, slot_of(chip)]
        return copy(PS.at[unit_rows(chip)], dst, leave("p"), enter("p"), at(1, chip // per))

    def send_p(chip):
        @pl.when((to_owner(chip) == nx - passes_on))
        def _():
            p_out(chip).start()

        @pl.when(to_owner(chip) == 2)
        def _():
            dev = at(1, lax.rem(x + passes_on, nx))
            dst = PV.at[slot_of(chip)]
            copy(PS.at[unit_rows(chip)], dst, leave("p"), pv_r.at[lax.rem(chip, per)], dev).start()

    def pass_on(chip):
        @pl.when(to_owner(chip) == passes_on)
        def _():
            slot = slot_of(chip)
            arrived(pv_r.at[lax.rem(chip, per)], PV.at[slot])
            r = unit_rows(chip)
            PS[r, :] = (PF[r, :] + PV[slot, :].astype(F32)).astype(BF16)
            p_out(chip).start()

    def handle(i):
        s = i // PIECES + 1
        h = lax.rem(i, PIECES)
        far = i >= full
        other = PIECES // 2
        hl = jnp.where(far, h + other, h)
        fr = lax.rem(z - s + nz, nz)
        fl = lax.rem(z + s, nz)
        third = i >= full - PIECES
        ring(True, fr, h, i).wait_recv()
        across(fr, h, jnp.where(far, nz - 1, 2 * s - 1)).start()

        @pl.when((i < full - PIECES) | (third & (h < other) & (i < full)))
        def _():
            ring(True, fr, h, i + PIECES).start()

        ring(False, fl, hl, i).wait_recv()
        across(fl, hl, jnp.where(far, nz - 1, 2 * s)).start()

        @pl.when((i < full - PIECES) | (third & (h >= other) & (i < full)))
        def _():
            ring(False, fl, hl, jnp.where(third, i + PIECES - other, i + PIECES)).start()

        @pl.when(i + EARLY < strips)
        def _():
            send_ct(i + EARLY, 0)

    def need_tokens(j):
        arrived(d_r.at[j], T.at[token_rows(chip_of(j), 1 - k, 0, rows)])

    def handle_range(low, high):
        def one(i, _):
            handle(i)
            return 0

        lax.fori_loop(low, high, one, 0)

    held = HELD

    def settle(j, _):
        c = chip_of(j)
        need_ct(c)
        scale_sum(c)
        backward(c)
        return 0

    def slice_weights():
        cols = pl.ds(pl.multiple_of(y * slab, slab), slab)
        wide = W.shape[1]
        low_rank_t = tn(B[...], A[:, cols])
        high = low_rank_t.astype(BF16)
        WX[:wide, :] = W[cols, :].astype(F32).T.astype(BF16)
        WX[wide : 2 * wide, :] = high
        WX[2 * wide :, :] = (low_rank_t - high.astype(F32)).astype(BF16)

    need_tokens(0)
    project(z)
    handle_range(0, PIECES // 4)
    low_rank()
    handle_range(PIECES // 4, 3 * PIECES // 4)
    slice_weights()
    handle_range(3 * PIECES // 4, PIECES)
    send_p(z)

    def turn(j, _):
        s = (j + 1) // 2
        odd = lax.rem(j, 2)
        chip = chip_of(j)

        @pl.when((odd == 1) & (j < nz - 3))
        def _():
            handle(s * PIECES)

        need_tokens(j)
        project(chip)

        @pl.when(j == 1)
        def _():
            arrived(enter("nx"), NX.at[pl.ds(0, nx - 1)])
            sq = NX[0]
            for i in range(1, nx):
                sq = sq + NX[i]
            norm = jnp.sqrt(sq + EPS)
            NORM[...] = norm
            SCALE[...] = MAG[...] / norm

        mid = s * PIECES + PIECES // 2
        low = jnp.minimum(jnp.where(odd == 1, s * PIECES + 1, mid), full)
        high = jnp.minimum(jnp.where(odd == 1, mid, mid + 1), full)
        low = jnp.where(j == nz - 3, full, low)
        high = jnp.where(j == nz - 3, pieces, high)
        handle_range(low, high)

        for level in range(max(levels.values())):

            @pl.when(j == level + 1)
            def _():
                spread_word(level)

        @pl.when(j < held)
        def _():
            send_p(chip)

        @pl.when((j >= 2) & (j < nz - 3))
        def _():
            settle(j - 2, 0)

        handle_range(high, jnp.where(odd == 1, high, jnp.minimum((s + 1) * PIECES, full)))

        @pl.when((j >= 2) & (j < nz - 3))
        def _():
            pass_on(chip_of(j - 2))

        @pl.when(j == nz - 4)
        def _():
            lax.fori_loop(nz - 5, nz - 3, settle, 0)
            for i in range(ny):
                H[i] = R[:, i * slab : (i + 1) * slab]
            R[...] = jnp.zeros_like(R)
            RY[y] = H[y]
            for d in far_first(ny):
                dst = lax.rem(y + d, ny)
                to_y("ry", H.at[dst], RY.at[y], d).start()

        return 0

    lax.fori_loop(1, nz - 1, turn, 0)
    for j in (nz - 3, nz - 2):
        need_ct(chip_of(j))
        scale_sum(chip_of(j))
    need_tokens(nz - 1)
    project(chip_of(nz - 1))

    need_ct(chip_of(nz - 1))
    scale_sum(chip_of(nz - 1))
    me = y * nx + x
    SS[me] = jnp.sum(SACC[...], axis=0, keepdims=True)
    away = [(dy, dx) for dy in range(ny) for dx in range(nx) if dy or dx]
    for dy, dx in sorted(away, key=lambda o: -min(o[0], ny - o[0]) - min(o[1], nx - o[1])):
        dev = (lax.rem(y + dy, ny), lax.rem(x + dx, nx), z, k)
        copy(SS.at[me], SS.at[me], leave("s"), enter("s"), dev).start()

    def finish_b(j, _):
        backward(chip_of(j))
        return 0

    lax.fori_loop(nz - 3, nz, finish_b, 0)
    for i in range(ny):
        HL[i] = R[:, i * slab : (i + 1) * slab].astype(BF16)
    RL[y] = HL[y]
    for d in far_first(ny):
        dst = lax.rem(y + d, ny)
        to_y("rl", HL.at[dst], RL.at[y], d).start()
    for i in range(nx):
        BGS[i] = BG[:, i * part : (i + 1) * part]
    BX[x] = BGS[x]

    for d in range(1, nx):
        dst = lax.rem(x + d, nx)
        to_x("bx", BGS.at[dst], BX.at[x], d).start()

    def send_held(j, _):
        send_p(chip_of(j))
        return 0

    lax.fori_loop(held, nz, send_held, 0)
    for j in (held - 2, held - 1):
        pass_on(chip_of(j))

    arrived(enter("ry"), RY.at[pl.ds(0, ny - 1)])
    row_part = RY[0]
    for i in range(1, ny):
        row_part = row_part + RY[i]
    norm = NORM[...]
    inverse = 1.0 / norm
    slope = -MAG[...] * (inverse * inverse * inverse)

    arrived(enter("s"), SS.at[pl.ds(0, nx * ny - 1)])
    s_all = SS[0]
    for i in range(1, nx * ny):
        s_all = s_all + SS[i]
    coef = s_all * slope
    scaled = (B[...].astype(F32) * coef).astype(BF16)
    part_y = nn(jnp.concatenate([scaled] * 3, axis=1), WX[...])
    arrived(enter("rl"), RL.at[pl.ds(0, ny - 1)])
    for i in range(ny):
        row_part = row_part + RL[i].astype(F32)
    part_y = part_y + row_part

    for i in range(2):
        CX[i] = part_y[:, i * lane : (i + 1) * lane].astype(BF16)
    here = 2 * z + k
    ZX[here] = CX[k]
    for d in far_first(nz) + [0]:
        for other in (0, 1):
            if d or other:
                core = k if other == 0 else 1 - k
                dev = (y, x, lax.rem(z + d, nz), core)
                copy(CX.at[core], ZX.at[here], leave("zx"), enter("zx"), dev).start()
    gmag_ref[...] = s_all * inverse

    def pass_held(j, _):
        pass_on(chip_of(j))
        return 0


    arrived(enter("bx"), BX.at[pl.ds(0, nx - 1)])
    bx = BX[0]
    for i in range(1, nx):
        bx = bx + BX[i]
    BY[y] = bx
    for d in far_first(ny):
        to_y("by", BY.at[y], BY.at[y], d).start()
    lax.fori_loop(held, nz, pass_held, 0)
    arrived(enter("ax"), AX.at[pl.ds(0, nx - 1)])
    a_all = AX[0]
    for i in range(1, nx):
        a_all = a_all + AX[i]

    arrived(enter("zx"), ZX.at[pl.ds(0, 2 * nz - 1)])
    whole = ZX[0].astype(F32)
    for i in range(1, 2 * nz):
        whole = whole + ZX[i].astype(F32)
    spot = 2 * y + k
    IF[spot] = whole.astype(BF16)
    for d in far_first(ny) + [0]:
        for other in (0, 1):
            if d or other:
                dev = (lax.rem(y + d, ny), x, z, k if other == 0 else 1 - k)
                copy(IF.at[spot], IF.at[spot], leave("if"), enter("if"), dev).start()

    arrived(enter("p"), PR)
    rest = pl.ds(pl.multiple_of(x * own, own), own)
    total = PF[rest, :]
    for side in range(2):
        total = total + PR[side].astype(F32)
    proj_ref[...] = (total * SCALE[...]).astype(BF16)

    arrived(enter("by"), BY.at[pl.ds(0, ny - 1)])
    b_all = BY[0]
    for i in range(1, ny):
        b_all = b_all + BY[i]

    for i in range(nx):

        @pl.when(x == i)
        def _():
            c = slice(i * part, (i + 1) * part)
            gb_ref[:, c] = b_all + a_all * coef[:, c]

    def gb_part(i):
        return gb_ref.at[:, pl.ds(pl.multiple_of(i * part, part), part)]

    for d in range(1, nx):
        to_x("bo", gb_part(x), gb_part(x), d).start()

    arrived(enter("bo"), gb_ref.at[:, pl.ds(0, (nx - 1) * part)])
    arrived(enter("if"), IF.at[pl.ds(0, 2 * ny - 1)])
    for i in range(2 * ny):
        ifg_ref[:, i * lane : (i + 1) * lane] = IF[i].astype(F32)

    def sent(name, ref):
        copy(ref, ref, leave(name), leave(name), partner).wait_send()

    sent("own", T.at[pl.ds(0, 4 * pieces * piece + rows)])
    sent("ct", CT.at[pl.ds(0, (nx - 1) * own)])
    sent("p", PS.at[pl.ds(0, (nx - 1) * own)])
    sent("nx", NX.at[pl.ds(0, nx - 1)])
    sent("ax", AX.at[pl.ds(0, nx - 1)])
    sent("s", SS.at[pl.ds(0, nx * ny - 1)])
    sent("bx", BX.at[pl.ds(0, nx - 1)])
    sent("by", BY.at[pl.ds(0, ny - 1)])
    sent("bo", gb_ref.at[:, pl.ds(0, (nx - 1) * part)])
    sent("ry", RY.at[pl.ds(0, ny - 1)])
    sent("rl", RL.at[pl.ds(0, ny - 1)])
    sent("zx", ZX.at[pl.ds(0, 2 * nz - 1)])
    sent("if", IF.at[pl.ds(0, 2 * ny - 1)])


def put_out(*refs):
    *pairs, sem = refs
    copies = [pltpu.make_async_copy(pairs[i], pairs[i + 4], sem.at[i]) for i in range(4)]
    for c in copies:
        c.start()
    for c in copies:
        c.wait()


def per_device(sizes, tokens, weight, a, b, magnitude, cotangent, lengths):
    ny, nx, nz = sizes
    rows, feats = tokens.shape
    rank, cols = b.shape
    group = rows * 2 * nz
    own = group // nx
    slab = feats // ny
    part = cols // nx
    per = nz // nx
    ring = (nz // 2 - 1) * PIECES + PIECES // 2
    words = ny // 2 + nx // 2 + nz // 2 - 2
    V = pltpu.VMEM
    S = lambda n: pltpu.SemaphoreType.DMA((n,))
    outs = pl.pallas_call(
        functools.partial(kernel, sizes),
        out_shape=(
            V((own, cols), BF16),
            V((1, cols), F32),
            V((rank, feats), F32),
            V((rank, cols), F32),
        ),
        in_specs=[pl.BlockSpec(memory_space=pl.ANY)] * 7,
        out_specs=[pl.BlockSpec(memory_space=pltpu.VMEM)] * 4,
        scratch_shapes=[
            V((group, feats), BF16),
            V((feats, cols), BF16),
            V((rank, feats), BF16),
            V((rank, cols), BF16),
            V((group, cols), BF16),
            V((group, 128), F32),
            V((group, cols), F32),
            V((group, cols), BF16),
            V((2, own, cols), BF16),
            V((own, cols), BF16),
            V((group, rank), BF16),
            V((nx, 1, cols), F32),
            V((nx, rank, part), F32),
            V((8, cols), F32),
            V((nx * ny, 1, cols), F32),
            V((1, cols), F32),
            V((1, cols), F32),
            V((rank, cols), F32),
            V((nx, rank, part), F32),
            V((nx, rank, part), F32),
            V((ny, rank, part), F32),
            V((rank, feats), F32),
            V((ny, rank, slab), F32),
            V((ny, rank, slab), F32),
            V((ny, rank, slab), BF16),
            V((ny, rank, slab), BF16),
            V((2, rank, slab // 2), BF16),
            V((2 * nz, rank, slab // 2), BF16),
            V((2 * ny, rank, slab // 2), BF16),
            V((nx, rank, part), F32),
            V((3 * cols, slab), BF16),
            V((feats, 128), BF16),
            V((1, cols), F32),
            pltpu.SMEM(lengths.shape, jnp.int32),
            S(6 + PIECES),
            S(ring), S(ring),
            S(nz), S(nz), S(per),
            S(len(LEAVE)), S(len(ENTER)),
            pltpu.SemaphoreType.REGULAR((words,)),
        ],
        compiler_params=pltpu.CompilerParams(
            collective_id=0, has_side_effects=True, vmem_limit_bytes=56 * 1024 * 1024
        ),
        name="lora_step",
    )(tokens, weight, a, b, magnitude.reshape(1, cols), cotangent, lengths)
    whole = [jax.ShapeDtypeStruct(o.shape, o.dtype) for o in outs]
    proj, gmag, ifg, gb = pl.pallas_call(
        put_out,
        out_shape=whole,
        in_specs=[pl.BlockSpec(memory_space=pltpu.VMEM)] * 4,
        out_specs=[pl.BlockSpec(memory_space=pl.ANY)] * 4,
        scratch_shapes=[S(4)],
        compiler_params=pltpu.CompilerParams(vmem_limit_bytes=1024 * 1024),
        name="put_out",
    )(*outs)
    return proj, gmag.reshape(cols), ifg, gb


def solution(mesh):
    ny, nx = mesh.shape["dp"], mesh.shape["row"]
    nz = mesh.shape["col"] // 2
    split = Mesh(mesh.devices.reshape(ny, nx, nz, 2), AXES)
    return jax.shard_map(
        functools.partial(per_device, (ny, nx, nz)),
        mesh=split,
        in_specs=(
            P(("dp", "z", "core"), "row"),
            P("row", COL),
            P(None, "row"),
            P(None, COL),
            P(COL),
            P(("dp", "row"), COL),
            P("dp", None),
        ),
        out_specs=(P(("dp", "row"), COL), P(COL), P(None, "row"), P(None, COL)),
        check_vma=False,
    )
```

```python
import functools

import jax
import jax.numpy as jnp
from jax import lax
from jax.experimental import pallas as pl
from jax.experimental.pallas import tpu as pltpu
from jax.sharding import Mesh
from jax.sharding import PartitionSpec as P

AXES = ("dp", "row", "z", "core")
COL = ("z", "core")
EPS = 1e-06
F32 = jnp.float32
BF16 = jnp.bfloat16
HIGHEST = lax.Precision.HIGHEST
HELD = 5
PIECES = 4
EARLY = 4


TOKEN = "own"
SAME = ("zr", "zl", "d", "own")
LEAVE = ("own", "ct", "p", "nx", "ax", "s", "bx", "by", "bo", "ry", "rl", "zx", "if")
ENTER = ("p", "nx", "ax", "s", "bx", "by", "bo", "ry", "rl", "zx", "if")


def nn(a, b):
    return lax.dot_general(a, b, (((1,), (0,)), ((), ())), preferred_element_type=F32)


def nt(a, b):
    return lax.dot_general(a, b, (((1,), (1,)), ((), ())), preferred_element_type=F32)


def tn(a, b):
    return lax.dot_general(a, b, (((0,), (0,)), ((), ())), preferred_element_type=F32)


def exact(a, b):
    return lax.dot_general(
        a, b, (((1,), (0,)), ((), ())), preferred_element_type=F32, precision=HIGHEST
    )


def far_first(n):
    return sorted(range(1, n), key=lambda d: -min(d, n - d))


def fold(a):
    return jnp.sum(a.reshape(a.shape[0] // 8, 8, a.shape[1]), axis=0)


def kernel(
    sizes,
    tok_hbm, w_hbm, a_hbm, b_hbm, mag_hbm, ct_hbm, lens_hbm,
    proj_ref, gmag_ref, ifg_ref, gb_ref,
    T, W, A, B, CT, WT, PF, PS, PR, PV, DB,
    NX, AX, SACC, SS, SCALE, NORM, BG, BGS, BX, BY, R, RY, H, RL, HL, CX, ZX, IF, AM, WX, AT, MAG, LENS,
    load_sem, zr_r, zl_r, d_r, ct_r, pv_r, out_sem, in_sem, wave,
):
    ny, nx, nz = sizes
    y, x, z, k = (lax.axis_index(a) for a in AXES)
    rows = tok_hbm.shape[0]
    piece = rows // PIECES
    unit = 2 * rows
    own = nz // nx * unit
    per = nz // nx
    slab = T.shape[1] // ny
    lane = slab // 2
    part = W.shape[1] // nx

    def at(axis, index):
        return tuple(index if i == axis else v for i, v in enumerate((y, x, z, k)))

    def step(axis, by, n):
        return at(axis, lax.rem((y, x, z)[axis] + by + n, n))

    def leave(name):
        return out_sem.at[LEAVE.index(TOKEN if name in SAME else name)]

    def enter(name):
        return in_sem.at[ENTER.index(name)]

    partner = (y, x, z, 1 - k)
    right = step(2, 1, nz)
    left = step(2, -1, nz)

    def copy(src, dst, ssem, rsem, dev):
        return pltpu.make_async_remote_copy(
            src_ref=src, dst_ref=dst, send_sem=ssem, recv_sem=rsem,
            device_id=dev, device_id_type=pl.DeviceIdType.MESH,
        )

    def arrived(sem, ref):
        copy(ref, ref, sem, sem, partner).wait_recv()

    def token_rows(chip, core, h, n):
        return pl.ds(pl.multiple_of(chip * unit + core * rows + h * piece, piece), n)

    mine = token_rows(z, k, 0, rows)
    owned = pl.ds(pl.multiple_of(x * own, own), own)
    loads = [
        pltpu.make_async_copy(ct_hbm, CT.at[owned], load_sem.at[0]),
        pltpu.make_async_copy(a_hbm, A, load_sem.at[1]),
        pltpu.make_async_copy(b_hbm, B, load_sem.at[2]),
        pltpu.make_async_copy(w_hbm, W, load_sem.at[3]),
        pltpu.make_async_copy(mag_hbm, MAG, load_sem.at[4]),
        pltpu.make_async_copy(lens_hbm, LENS, load_sem.at[5]),
    ]
    first = [
        pltpu.make_async_copy(
            tok_hbm.at[pl.ds(h * piece, piece)], T.at[token_rows(z, k, h, piece)], load_sem.at[6 + h]
        )
        for h in range(PIECES)
    ]
    for c in first + loads:
        c.start()

    barrier = pltpu.get_barrier_semaphore()
    near = [partner] + [step(axis, d, n) for axis, n in ((2, nz), (1, nx), (0, ny)) for d in (1, -1)]

    def signal(sem, dev):
        pl.semaphore_signal(sem, inc=1, device_id=dev, device_id_type=pl.DeviceIdType.MESH)

    for dev in near:
        signal(barrier, dev)

    seqs = LENS.shape[1]

    def weigh(i, _):
        pos = lax.broadcasted_iota(jnp.int32, (unit, 128), 0) + i * unit
        total = jnp.zeros((unit, 128), F32)
        start = jnp.int32(0)
        for s in range(seqs):
            length = LENS[0, s]
            end = start + length
            inverse = 1.0 / jnp.full((1, 128), length, jnp.int32).astype(F32)
            total += jnp.where((pos >= start) & (pos < end), inverse, 0.0)
            start = end
        WT[pl.ds(pl.multiple_of(i * unit, unit), unit), :] = total
        return 0

    pl.semaphore_wait(barrier, len(near))

    def ring(right_way, src_chip, h, idx):
        r = token_rows(src_chip, k, h, piece)
        if right_way:
            return copy(T.at[r], T.at[r], leave("zr"), zr_r.at[idx], right)
        return copy(T.at[r], T.at[r], leave("zl"), zl_r.at[idx], left)

    def across(src_chip, h, j):
        r = token_rows(src_chip, k, h, piece)
        return copy(T.at[r], T.at[r], leave("d"), d_r.at[j], partner)

    full = (nz // 2 - 1) * PIECES
    pieces = full + PIECES // 2
    for h in range(PIECES):
        first[h].wait()
        if h < PIECES // 2:
            ring(True, z, h, h).start()
            ring(False, z, h, h).start()

    def rest_of_own():
        for h in range(PIECES // 2, PIECES):
            ring(True, z, h, h).start()
            ring(False, z, h, h).start()

    @pl.when(k == 0)
    def _():
        rest_of_own()

    copy(T.at[mine], T.at[mine], leave("own"), d_r.at[0], partner).start()

    levels = {0: ny // 2, 1: nx // 2 - 1, 2: nz // 2 - 1}
    base = {1: 0, 0: levels[1], 2: levels[1] + levels[0]}

    def tell(axis, level):
        for d in (1, -1):
            signal(wave.at[base[axis] + level], step(axis, d, (ny, nx, nz)[axis]))

    def hear(axis, level):
        pl.semaphore_wait(wave.at[base[axis] + level], 2)

    tell(1, 0)
    tell(2, 0)
    loads[5].wait()
    lax.fori_loop(0, nz, weigh, 0)

    @pl.when(k == 1)
    def _():
        rest_of_own()

    def spread_word(level):
        for axis in (0, 2):
            if level < levels[axis]:
                hear(axis, level)
            if level + 1 < levels[axis]:
                tell(axis, level + 1)

    def chip_of(j):
        s = (j + 1) // 2
        return lax.rem(z + nz + jnp.where(lax.rem(j, 2) == 1, -s, s), nz)

    def unit_rows(chip):
        return pl.ds(pl.multiple_of(chip * unit, unit), unit)

    def turn_of(chip):
        d = lax.rem(chip - z + nz, nz)
        return jnp.where(d < nz // 2, 2 * d, 2 * (nz - d) - 1)

    ahead = jnp.where(turn_of(x * per) < turn_of(x * per + 1), 0, 1)
    strip = unit // 2
    strips = per * 2 * (nx - 1)

    def ct_copy(loc, part_of, dx, src_x):
        r = pl.ds(pl.multiple_of((src_x * per + loc) * unit + part_of * strip, strip), strip)
        d = lax.rem(dx - src_x + nx, nx)
        return copy(CT.at[r], CT.at[r], leave("ct"), ct_r.at[src_x * per + loc], at(1, dx))

    def send_ct(n, _):
        u = n // (strips // per)
        loc = jnp.where(u == 0, ahead, 1 - ahead)
        m = lax.rem(n, strips // per)
        ct_copy(loc, m // (nx - 1), lax.rem(x + 1 + lax.rem(m, nx - 1), nx), x).start()
        return 0

    for c in loads[1:5]:
        c.wait()
    chunk = slab

    def norm_part(i, acc):
        c = pl.ds(pl.multiple_of(i * chunk, chunk), chunk)
        m = W[c, :].astype(F32) + tn(A[:, c], B[...])
        return acc + fold(m * m)

    acc = lax.fori_loop(0, ny, norm_part, jnp.zeros((8, W.shape[1]), F32), unroll=4)
    NX[x] = jnp.sum(acc, axis=0, keepdims=True)
    for level in range(levels[1]):
        hear(1, level)
        if level + 1 < levels[1]:
            tell(1, level + 1)
    tell(0, 0)
    loads[0].wait()

    def to_x(name, src, slot, d):
        return copy(src, slot, leave(name), enter(name), step(1, d, nx))

    def to_y(name, src, slot, d):
        return copy(src, slot, leave(name), enter(name), step(0, d, ny))

    for d in range(1, nx):
        to_x("nx", NX.at[x], NX.at[x], d).start()
    lax.fori_loop(0, EARLY, send_ct, 0)

    wide_a = jnp.concatenate([A[...].astype(F32), jnp.zeros((128 - A.shape[0], A.shape[1]), F32)], axis=0)
    AT[...] = wide_a.T.astype(BF16)
    SACC[...] = jnp.zeros_like(SACC)
    BG[...] = jnp.zeros_like(BG)
    R[...] = jnp.zeros_like(R)

    def low_rank():
        am = nn(A[...], W[...]) + exact(nt(A[...], A[...]), B[...].astype(F32))
        for i in range(nx):
            AM[i] = am[:, i * part : (i + 1) * part]
        AX[x] = AM[x]
        for d in range(1, nx):
            dst = lax.rem(x + d, nx)
            to_x("ax", AM.at[dst], AX.at[x], d).start()

    def project(chip):
        r = unit_rows(chip)
        t = T[r, :]
        down = nn(t, AT[...])[:, : A.shape[0]].astype(BF16)
        p = nn(t, W[...]) + nn(down, B[...])
        DB[r, :] = down
        PF[r, :] = p
        PS[r, :] = p.astype(BF16)

    def need_ct(chip):
        @pl.when(chip // per != x)
        def _():
            arrived(ct_r.at[chip], CT.at[unit_rows(chip)])

    def weighted(chip):
        r = unit_rows(chip)
        w = WT[r, :]
        return CT[r, :].astype(F32) * jnp.concatenate([w] * (W.shape[1] // 128), axis=1)

    def scale_sum(chip):
        SACC[...] += fold(weighted(chip) * PF[unit_rows(chip), :])

    def backward(chip):
        r = unit_rows(chip)
        gp = (weighted(chip) * SCALE[...]).astype(BF16)
        BG[...] += tn(DB[r, :], gp)
        back = nt(B[...], gp)
        high = back.astype(BF16)
        low = (back - high.astype(F32)).astype(BF16)
        both = nn(jnp.concatenate([high, low], axis=0), T[r, :])
        R[...] += both[: back.shape[0]] + both[back.shape[0] :]

    def to_owner(chip):
        return lax.rem(chip // per - x + nx, nx)

    passes_on = jnp.where(k == 0, 1, nx - 1)

    def slot_of(chip):
        return pl.ds(pl.multiple_of(lax.rem(chip, per) * unit, unit), unit)

    def p_out(chip):
        side = jnp.where(to_owner(chip) == 1, 0, 1)
        dst = PR.at[side, slot_of(chip)]
        return copy(PS.at[unit_rows(chip)], dst, leave("p"), enter("p"), at(1, chip // per))

    def send_p(chip):
        @pl.when((to_owner(chip) == nx - passes_on))
        def _():
            p_out(chip).start()

        @pl.when(to_owner(chip) == 2)
        def _():
            dev = at(1, lax.rem(x + passes_on, nx))
            dst = PV.at[slot_of(chip)]
            copy(PS.at[unit_rows(chip)], dst, leave("p"), pv_r.at[lax.rem(chip, per)], dev).start()

    def pass_on(chip):
        @pl.when(to_owner(chip) == passes_on)
        def _():
            slot = slot_of(chip)
            arrived(pv_r.at[lax.rem(chip, per)], PV.at[slot])
            r = unit_rows(chip)
            PS[r, :] = (PF[r, :] + PV[slot, :].astype(F32)).astype(BF16)
            p_out(chip).start()

    def handle(i):
        s = i // PIECES + 1
        h = lax.rem(i, PIECES)
        far = i >= full
        other = PIECES // 2
        hl = jnp.where(far, h + other, h)
        fr = lax.rem(z - s + nz, nz)
        fl = lax.rem(z + s, nz)
        third = i >= full - PIECES
        ring(True, fr, h, i).wait_recv()
        across(fr, h, jnp.where(far, nz - 1, 2 * s - 1)).start()

        @pl.when((i < full - PIECES) | (third & (h < other) & (i < full)))
        def _():
            ring(True, fr, h, i + PIECES).start()

        ring(False, fl, hl, i).wait_recv()
        across(fl, hl, jnp.where(far, nz - 1, 2 * s)).start()

        @pl.when((i < full - PIECES) | (third & (h >= other) & (i < full)))
        def _():
            ring(False, fl, hl, jnp.where(third, i + PIECES - other, i + PIECES)).start()

        @pl.when(i + EARLY < strips)
        def _():
            send_ct(i + EARLY, 0)

    def need_tokens(j):
        arrived(d_r.at[j], T.at[token_rows(chip_of(j), 1 - k, 0, rows)])

    def handle_range(low, high):
        def one(i, _):
            handle(i)
            return 0

        lax.fori_loop(low, high, one, 0)

    held = HELD

    def settle(j, _):
        c = chip_of(j)
        need_ct(c)
        scale_sum(c)
        backward(c)
        return 0

    def slice_weights():
        cols = pl.ds(pl.multiple_of(y * slab, slab), slab)
        wide = W.shape[1]
        low_rank_t = tn(B[...], A[:, cols])
        high = low_rank_t.astype(BF16)
        WX[:wide, :] = W[cols, :].astype(F32).T.astype(BF16)
        WX[wide : 2 * wide, :] = high
        WX[2 * wide :, :] = (low_rank_t - high.astype(F32)).astype(BF16)

    need_tokens(0)
    project(z)
    handle_range(0, PIECES // 4)
    low_rank()
    handle_range(PIECES // 4, 3 * PIECES // 4)
    slice_weights()
    handle_range(3 * PIECES // 4, PIECES)
    send_p(z)

    def turn(j, _):
        s = (j + 1) // 2
        odd = lax.rem(j, 2)
        chip = chip_of(j)

        @pl.when((odd == 1) & (j < nz - 3))
        def _():
            handle(s * PIECES)

        need_tokens(j)
        project(chip)

        @pl.when(j == 1)
        def _():
            arrived(enter("nx"), NX.at[pl.ds(0, nx - 1)])
            sq = NX[0]
            for i in range(1, nx):
                sq = sq + NX[i]
            norm = jnp.sqrt(sq + EPS)
            NORM[...] = norm
            SCALE[...] = MAG[...] / norm

        mid = s * PIECES + PIECES // 2
        low = jnp.minimum(jnp.where(odd == 1, s * PIECES + 1, mid), full)
        high = jnp.minimum(jnp.where(odd == 1, mid, mid + 1), full)
        low = jnp.where(j == nz - 3, full, low)
        high = jnp.where(j == nz - 3, pieces, high)
        handle_range(low, high)

        for level in range(max(levels.values())):

            @pl.when(j == level + 1)
            def _():
                spread_word(level)

        @pl.when(j < held)
        def _():
            send_p(chip)

        @pl.when((j >= 2) & (j < nz - 3))
        def _():
            settle(j - 2, 0)

        handle_range(high, jnp.where(odd == 1, high, jnp.minimum((s + 1) * PIECES, full)))

        @pl.when((j >= 2) & (j < nz - 3))
        def _():
            pass_on(chip_of(j - 2))

        @pl.when(j == nz - 4)
        def _():
            lax.fori_loop(nz - 5, nz - 3, settle, 0)
            for i in range(ny):
                H[i] = R[:, i * slab : (i + 1) * slab]
            R[...] = jnp.zeros_like(R)
            RY[y] = H[y]
            for d in far_first(ny):
                dst = lax.rem(y + d, ny)
                to_y("ry", H.at[dst], RY.at[y], d).start()

        return 0

    lax.fori_loop(1, nz - 1, turn, 0)
    for j in (nz - 3, nz - 2):
        need_ct(chip_of(j))
        scale_sum(chip_of(j))
    need_tokens(nz - 1)
    project(chip_of(nz - 1))

    need_ct(chip_of(nz - 1))
    scale_sum(chip_of(nz - 1))
    me = y * nx + x
    SS[me] = jnp.sum(SACC[...], axis=0, keepdims=True)
    away = [(dy, dx) for dy in range(ny) for dx in range(nx) if dy or dx]
    for dy, dx in sorted(away, key=lambda o: -min(o[0], ny - o[0]) - min(o[1], nx - o[1])):
        dev = (lax.rem(y + dy, ny), lax.rem(x + dx, nx), z, k)
        copy(SS.at[me], SS.at[me], leave("s"), enter("s"), dev).start()

    def finish_b(j, _):
        backward(chip_of(j))
        return 0

    lax.fori_loop(nz - 3, nz, finish_b, 0)
    for i in range(ny):
        HL[i] = R[:, i * slab : (i + 1) * slab].astype(BF16)
    RL[y] = HL[y]
    for d in far_first(ny):
        dst = lax.rem(y + d, ny)
        to_y("rl", HL.at[dst], RL.at[y], d).start()
    for i in range(nx):
        BGS[i] = BG[:, i * part : (i + 1) * part]
    BX[x] = BGS[x]

    for d in range(1, nx):
        dst = lax.rem(x + d, nx)
        to_x("bx", BGS.at[dst], BX.at[x], d).start()

    def send_held(j, _):
        send_p(chip_of(j))
        return 0

    lax.fori_loop(held, nz, send_held, 0)
    for j in (held - 2, held - 1):
        pass_on(chip_of(j))

    arrived(enter("ry"), RY.at[pl.ds(0, ny - 1)])
    row_part = RY[0]
    for i in range(1, ny):
        row_part = row_part + RY[i]
    norm = NORM[...]
    inverse = 1.0 / norm
    slope = -MAG[...] * (inverse * inverse * inverse)

    arrived(enter("s"), SS.at[pl.ds(0, nx * ny - 1)])
    s_all = SS[0]
    for i in range(1, nx * ny):
        s_all = s_all + SS[i]
    coef = s_all * slope
    scaled = (B[...].astype(F32) * coef).astype(BF16)
    part_y = nn(jnp.concatenate([scaled] * 3, axis=1), WX[...])
    arrived(enter("rl"), RL.at[pl.ds(0, ny - 1)])
    for i in range(ny):
        row_part = row_part + RL[i].astype(F32)
    part_y = part_y + row_part

    for i in range(2):
        CX[i] = part_y[:, i * lane : (i + 1) * lane].astype(BF16)
    here = 2 * z + k
    ZX[here] = CX[k]
    for d in far_first(nz) + [0]:
        for other in (0, 1):
            if d or other:
                core = k if other == 0 else 1 - k
                dev = (y, x, lax.rem(z + d, nz), core)
                copy(CX.at[core], ZX.at[here], leave("zx"), enter("zx"), dev).start()
    gmag_ref[...] = s_all * inverse

    def pass_held(j, _):
        pass_on(chip_of(j))
        return 0


    arrived(enter("bx"), BX.at[pl.ds(0, nx - 1)])
    bx = BX[0]
    for i in range(1, nx):
        bx = bx + BX[i]
    BY[y] = bx
    for d in far_first(ny):
        to_y("by", BY.at[y], BY.at[y], d).start()
    lax.fori_loop(held, nz, pass_held, 0)
    arrived(enter("ax"), AX.at[pl.ds(0, nx - 1)])
    a_all = AX[0]
    for i in range(1, nx):
        a_all = a_all + AX[i]

    arrived(enter("zx"), ZX.at[pl.ds(0, 2 * nz - 1)])
    whole = ZX[0].astype(F32)
    for i in range(1, 2 * nz):
        whole = whole + ZX[i].astype(F32)
    spot = 2 * y + k
    IF[spot] = whole.astype(BF16)
    for d in far_first(ny) + [0]:
        for other in (0, 1):
            if d or other:
                dev = (lax.rem(y + d, ny), x, z, k if other == 0 else 1 - k)
                copy(IF.at[spot], IF.at[spot], leave("if"), enter("if"), dev).start()

    arrived(enter("p"), PR)
    rest = pl.ds(pl.multiple_of(x * own, own), own)
    total = PF[rest, :]
    for side in range(2):
        total = total + PR[side].astype(F32)
    proj_ref[...] = (total * SCALE[...]).astype(BF16)

    arrived(enter("by"), BY.at[pl.ds(0, ny - 1)])
    b_all = BY[0]
    for i in range(1, ny):
        b_all = b_all + BY[i]

    for i in range(nx):

        @pl.when(x == i)
        def _():
            c = slice(i * part, (i + 1) * part)
            gb_ref[:, c] = b_all + a_all * coef[:, c]

    def gb_part(i):
        return gb_ref.at[:, pl.ds(pl.multiple_of(i * part, part), part)]

    for d in range(1, nx):
        to_x("bo", gb_part(x), gb_part(x), d).start()

    arrived(enter("bo"), gb_ref.at[:, pl.ds(0, (nx - 1) * part)])
    arrived(enter("if"), IF.at[pl.ds(0, 2 * ny - 1)])
    for i in range(2 * ny):
        ifg_ref[:, i * lane : (i + 1) * lane] = IF[i].astype(F32)

    def sent(name, ref):
        copy(ref, ref, leave(name), leave(name), partner).wait_send()

    sent("own", T.at[pl.ds(0, 4 * pieces * piece + rows)])
    sent("ct", CT.at[pl.ds(0, (nx - 1) * own)])
    sent("p", PS.at[pl.ds(0, (nx - 1) * own)])
    sent("nx", NX.at[pl.ds(0, nx - 1)])
    sent("ax", AX.at[pl.ds(0, nx - 1)])
    sent("s", SS.at[pl.ds(0, nx * ny - 1)])
    sent("bx", BX.at[pl.ds(0, nx - 1)])
    sent("by", BY.at[pl.ds(0, ny - 1)])
    sent("bo", gb_ref.at[:, pl.ds(0, (nx - 1) * part)])
    sent("ry", RY.at[pl.ds(0, ny - 1)])
    sent("rl", RL.at[pl.ds(0, ny - 1)])
    sent("zx", ZX.at[pl.ds(0, 2 * nz - 1)])
    sent("if", IF.at[pl.ds(0, 2 * ny - 1)])


def put_out(*refs):
    *pairs, sem = refs
    copies = [pltpu.make_async_copy(pairs[i], pairs[i + 4], sem.at[i]) for i in range(4)]
    for c in copies:
        c.start()
    for c in copies:
        c.wait()


def per_device(sizes, tokens, weight, a, b, magnitude, cotangent, lengths):
    ny, nx, nz = sizes
    rows, feats = tokens.shape
    rank, cols = b.shape
    group = rows * 2 * nz
    own = group // nx
    slab = feats // ny
    part = cols // nx
    per = nz // nx
    ring = (nz // 2 - 1) * PIECES + PIECES // 2
    words = ny // 2 + nx // 2 + nz // 2 - 2
    V = pltpu.VMEM
    S = lambda n: pltpu.SemaphoreType.DMA((n,))
    outs = pl.pallas_call(
        functools.partial(kernel, sizes),
        out_shape=(
            V((own, cols), BF16),
            V((1, cols), F32),
            V((rank, feats), F32),
            V((rank, cols), F32),
        ),
        in_specs=[pl.BlockSpec(memory_space=pl.ANY)] * 7,
        out_specs=[pl.BlockSpec(memory_space=pltpu.VMEM)] * 4,
        scratch_shapes=[
            V((group, feats), BF16),
            V((feats, cols), BF16),
            V((rank, feats), BF16),
            V((rank, cols), BF16),
            V((group, cols), BF16),
            V((group, 128), F32),
            V((group, cols), F32),
            V((group, cols), BF16),
            V((2, own, cols), BF16),
            V((own, cols), BF16),
            V((group, rank), BF16),
            V((nx, 1, cols), F32),
            V((nx, rank, part), F32),
            V((8, cols), F32),
            V((nx * ny, 1, cols), F32),
            V((1, cols), F32),
            V((1, cols), F32),
            V((rank, cols), F32),
            V((nx, rank, part), F32),
            V((nx, rank, part), F32),
            V((ny, rank, part), F32),
            V((rank, feats), F32),
            V((ny, rank, slab), F32),
            V((ny, rank, slab), F32),
            V((ny, rank, slab), BF16),
            V((ny, rank, slab), BF16),
            V((2, rank, slab // 2), BF16),
            V((2 * nz, rank, slab // 2), BF16),
            V((2 * ny, rank, slab // 2), BF16),
            V((nx, rank, part), F32),
            V((3 * cols, slab), BF16),
            V((feats, 128), BF16),
            V((1, cols), F32),
            pltpu.SMEM(lengths.shape, jnp.int32),
            S(6 + PIECES),
            S(ring), S(ring),
            S(nz), S(nz), S(per),
            S(len(LEAVE)), S(len(ENTER)),
            pltpu.SemaphoreType.REGULAR((words,)),
        ],
        compiler_params=pltpu.CompilerParams(
            collective_id=0, has_side_effects=True, vmem_limit_bytes=56 * 1024 * 1024
        ),
        name="lora_step",
    )(tokens, weight, a, b, magnitude.reshape(1, cols), cotangent, lengths)
    whole = [jax.ShapeDtypeStruct(o.shape, o.dtype) for o in outs]
    proj, gmag, ifg, gb = pl.pallas_call(
        put_out,
        out_shape=whole,
        in_specs=[pl.BlockSpec(memory_space=pltpu.VMEM)] * 4,
        out_specs=[pl.BlockSpec(memory_space=pl.ANY)] * 4,
        scratch_shapes=[S(4)],
        compiler_params=pltpu.CompilerParams(vmem_limit_bytes=1024 * 1024),
        name="put_out",
    )(*outs)
    return proj, gmag.reshape(cols), ifg, gb


def solution(mesh):
    ny, nx = mesh.shape["dp"], mesh.shape["row"]
    nz = mesh.shape["col"] // 2
    split = Mesh(mesh.devices.reshape(ny, nx, nz, 2), AXES)
    return jax.shard_map(
        functools.partial(per_device, (ny, nx, nz)),
        mesh=split,
        in_specs=(
            P(("dp", "z", "core"), "row"),
            P("row", COL),
            P(None, "row"),
            P(None, COL),
            P(COL),
            P(("dp", "row"), COL),
            P("dp", None),
        ),
        out_specs=(P(("dp", "row"), COL), P(COL), P(None, "row"), P(None, COL)),
        check_vma=False,
    )
```
